256 devices in a mesh: layer: 16 (over y, x_hi, core), row: 16 (over z, x_lo).
Axes of the slice: x: 4 (x_hi: 2, x_lo: 2; x = x_hi * 2 + x_lo), y: 4, z: 8, core: 2. Of those that a mesh axis runs over, the one named last changes fastest.
Arguments:
- magnet: float32 [3, 16, 1024, 1024], P(None, 'layer', 'row'), may hold values from -1 to 1, as said below
- saturation: float32 [16], P('layer'), may hold values from 0.5 to 2
- stiffness: float32 [16], P('layer'), may hold values from 0.1 to 0.4
- damping: float32 [16], P('layer'), may hold values from 0.02 to 0.5
- interface_sign: int32 [16, 2], P('layer'), may hold values from -1 to 1, as said below
Outputs:
- torque: float32 [3, 16, 1024, 1024], P(None, 'layer', 'row')
The draws below stay inside these ranges and needn't reach their ends.
Inputs may be any that keep to these rules, and one draw needn't show every extreme that they name: `magnet`: the three components of every cell form a unit vector. Every entry is -1 or 1; interface_sign[l, 1] equals interface_sign[l + 1, 0], the sign of the interface between layers l and l + 1; interface_sign[0, 0] and interface_sign[15, 1] belong to no interface.
All inputs are finite; a program needn't handle non-finite values.
Results may differ from the reference program's by a relative error of at most 0.0003.
Values sent between devices are 32-bit elements; how exact they have to be, the bound alone decides.
A program may use at most 128 MiB of HBM per device.

```python
import math
import jax
import jax.numpy as jnp
from jax import lax

NX = 1024
NY = 1024
LAYERS = 16


def draw_magnet(key, part):
    raw_field = jax.random.normal(key, (3, LAYERS, NY, NX), jnp.float32)
    return raw_field / jnp.sqrt(jnp.sum(raw_field * raw_field, axis=0, keepdims=True) + 1e-12)


def draw_interface_sign(key, part):
    coin_bits = jax.random.randint(jax.random.fold_in(key, 7), (LAYERS + 1,), 0, 2)
    values = 2 * coin_bits - 1
    return jnp.stack([values[:-1], values[1:]], axis=1).astype(jnp.int32)


def block_levels(own_key, dims, split, smallest, high):
    factor_of = 1.0
    for dim, blocks in split:
        heights = jax.random.uniform(jax.random.fold_in(jax.random.fold_in(own_key, 6), dim), (blocks,), jnp.float32, smallest / len(split), high / len(split))
        factor_of = factor_of * jnp.repeat(jnp.exp(heights), dims[dim] // blocks).reshape((-1,) + (1,) * (len(dims) - 1 - dim))
    return factor_of


def setup_inputs(seed: int = 0) -> dict:
    key_list = jax.random.split(jax.random.key(seed), 6)
    return {
        "magnet": draw_magnet(jax.random.fold_in(key_list[5], 71), 0),
        "saturation": jnp.clip(jnp.exp(math.log(2.0) - 1.3862944 * jax.random.uniform(key_list[1], (LAYERS,), jnp.float32) ** block_levels(key_list[1], (LAYERS,), ((0, 16),), -0.2, 0.2)), 0.5, 2.0),
        "stiffness": jnp.clip(jnp.exp(math.log(0.4) - 1.3862944 * jax.random.uniform(key_list[2], (LAYERS,), jnp.float32) ** block_levels(key_list[2], (LAYERS,), ((0, 16),), -0.2, 0.2)), 0.1, 0.4),
        "damping": jnp.clip(jnp.exp(math.log(0.5) - 3.218876 * jax.random.uniform(key_list[3], (LAYERS,), jnp.float32) ** block_levels(key_list[3], (LAYERS,), ((0, 16),), -0.2, 0.2)), 0.02, 0.5),
        "interface_sign": draw_interface_sign(jax.random.fold_in(key_list[5], 71), 0),
    }


THICKNESS = 1.0
LAYER_PITCH = 1.5
RKKY_STRENGTH = 0.8

def wave_numbers(length):
    position = jnp.arange(length, dtype=jnp.int32)
    position = jnp.where(position < length // 2, position, position - length)
    return 2.0 * jnp.pi / length * position.astype(jnp.float32)

def cross_product(vector_one, vector_two):
    return jnp.stack([vector_one[1] * vector_two[2] - vector_one[2] * vector_two[1], vector_one[2] * vector_two[0] - vector_one[0] * vector_two[2], vector_one[0] * vector_two[1] - vector_one[1] * vector_two[0]])

def reference(magnet, saturation, stiffness, damping, interface_sign):
    wave_y = wave_numbers(NY)[:, None]
    wave_x = wave_numbers(NX)[None, :]
    square = wave_x * wave_x + wave_y * wave_y
    anchor = square == 0.0
    wave_norm = jnp.sqrt(jnp.where(anchor, 1.0, square))
    unit_x = jnp.where(anchor, 0.0, wave_x / wave_norm)
    unit_y = jnp.where(anchor, 0.0, wave_y / wave_norm)
    self_z = jnp.where(anchor, 1.0, -jnp.expm1(-THICKNESS * wave_norm) / (THICKNESS * wave_norm))
    form_factor = jnp.where(anchor, 0.0, jnp.expm1(-THICKNESS * wave_norm) ** 2 / (2.0 * THICKNESS * wave_norm))
    spectra = jnp.fft.fft2(magnet * saturation[None, :, None, None], axes=(2, 3))
    along_wave = unit_x * spectra[0] + unit_y * spectra[1]
    normal = spectra[2]
    layer_ids = jnp.arange(LAYERS, dtype=jnp.int32)

    def one_layer(target):
        layer_gap = target - layer_ids
        distance = jnp.abs(layer_gap).astype(jnp.float32)[:, None, None]
        gap_sign = jnp.sign(layer_gap).astype(jnp.float32)[:, None, None]
        weight = jnp.where((layer_gap == 0)[:, None, None], 0.0, form_factor * jnp.exp(-wave_norm * (LAYER_PITCH * distance - THICKNESS)))
        psi_part = lax.optimization_barrier(jnp.sum(weight * (along_wave - 1j * gap_sign * normal), axis=0))
        chi_part = lax.optimization_barrier(jnp.sum(weight * (normal + 1j * gap_sign * along_wave), axis=0))
        return (psi_part, chi_part)
    psi_sum, chi_sum = lax.map(one_layer, layer_ids)
    psi_total = psi_sum + (1.0 - self_z) * along_wave
    chi_total = chi_sum + self_z * normal
    field_spectra = jnp.stack([-unit_x * psi_total, -unit_y * psi_total, -chi_total])
    demag_field = jnp.real(jnp.fft.ifft2(field_spectra, axes=(2, 3)))
    laplace = jnp.roll(magnet, 1, 2) + jnp.roll(magnet, -1, 2) + jnp.roll(magnet, 1, 3) + jnp.roll(magnet, -1, 3) - 4.0 * magnet
    exchange_field = stiffness[None, :, None, None] * laplace
    zero_layer = jnp.zeros_like(magnet[:, :1])
    layer_below = jnp.concatenate([zero_layer, magnet[:, :-1]], axis=1)
    layer_above = jnp.concatenate([magnet[:, 1:], zero_layer], axis=1)
    sign_value = interface_sign.astype(jnp.float32)
    rkky_field = RKKY_STRENGTH * (sign_value[None, :, 0, None, None] * layer_below + sign_value[None, :, 1, None, None] * layer_above)
    total_field = demag_field + exchange_field + rkky_field
    precess = cross_product(magnet, total_field)
    relax_term = cross_product(magnet, precess)
    damping_now = damping[None, :, None, None]
    return -(precess + damping_now * relax_term) / (1.0 + damping_now * damping_now)
```

```python
import functools
import math

import jax
import jax.numpy as jnp
import numpy as np
from jax import lax
from jax.experimental import pallas as pl
from jax.experimental.pallas import tpu as pltpu
from jax.sharding import PartitionSpec as P

N = 1024
HALF = N // 2
BINS = N // 4
LAYERS = 16
ROWS = 64
DEVICES = 256
THICKNESS = 1.0
LAYER_PITCH = 1.5
RKKY_STRENGTH = 0.8
F32 = jnp.float32
BF16 = jnp.bfloat16
NT = (((1,), (1,)), ((), ()))
NN = (((1,), (0,)), ((), ()))
TN = (((0,), (0,)), ((), ()))


def wave_tables():
    grid = np.arange(HALF)
    bins = np.arange(BINS)
    tables = []
    for parity in range(2):
        phase = (2 * bins[:, None] + parity) * grid[None, :] % N * (2.0 * np.pi / N)
        cosines, sines = np.cos(phase), np.sin(phase)
        if parity == 0:
            sines[0] = 1.0 - 2.0 * (grid % 2)
        tables.append(np.concatenate([cosines, sines], axis=0))
    exact = np.stack(tables)
    high = exact.astype(np.dtype(BF16))
    low = (exact - high.astype(np.float64)).astype(np.dtype(BF16))
    return jnp.asarray(high), jnp.asarray(low)


def split(value):
    high = value.astype(BF16)
    return high, (value - high.astype(F32)).astype(BF16)


def product(left, right, dims):
    (left_high, left_low), (right_high, right_low) = left, right
    dot = functools.partial(lax.dot_general, dimension_numbers=dims, preferred_element_type=F32)
    return dot(left_high, right_high) + (dot(left_high, right_low) + dot(left_low, right_high))


def lane_low(shape):
    return lax.broadcasted_iota(jnp.int32, shape, len(shape) - 1) < ROWS


def forward_x_kernel(sat_ref, stiff_ref, sign_ref, magnet_ref, high_ref, low_ref, out_ref):
    left, right = magnet_ref[:, :HALF], magnet_ref[:, HALF:]
    low_half = lane_low((DEVICES, 128))
    first = lax.broadcasted_iota(jnp.int32, (DEVICES, 128), 0) == 0
    for slot in range(2):
        folded = left - right if slot else left + right
        folded = jnp.concatenate([folded, folded[2 * ROWS :]], axis=0)
        waves = product((high_ref[slot], low_ref[slot]), split(folded), NT)
        cosine, sine = waves[:BINS], waves[BINS:]
        one, two = cosine[:, :128], sine[:, :128]
        if slot == 0:
            x_one, x_two = jnp.where(first, two, one), jnp.where(first, one, two)
        else:
            x_one, x_two = one, two
        out_ref[pl.ds(slot, DEVICES, stride=8), :] = jnp.where(low_half, x_one, -two)
        out_ref[pl.ds(2 + slot, DEVICES, stride=8), :] = jnp.where(low_half, x_two, one)
        out_ref[pl.ds(4 + slot, DEVICES, stride=8), :] = jnp.where(
            low_half, -sine[:, 128:], cosine[:, 128:]
        )
    even = lax.rem(lax.axis_index("row"), 2) == 0
    six = jnp.where(even, sat_ref[0], sign_ref[0, 0].astype(F32))
    seven = jnp.where(even, stiff_ref[0], sign_ref[0, 1].astype(F32))
    out_ref[pl.ds(6, DEVICES, stride=8), :] = jnp.full((DEVICES, 128), six, F32)
    out_ref[pl.ds(7, DEVICES, stride=8), :] = jnp.full((DEVICES, 128), seven, F32)


def symbols(device, parity, tile, sine):
    shape = (8, 128)
    row = lax.broadcasted_iota(jnp.int32, shape, 0)
    slot, word = row % 2, row // 2 % 2
    bin_y = 2 * (lax.broadcasted_iota(jnp.int32, shape, 1) + 128 * tile) + parity
    if sine and parity == 0:
        bin_y = jnp.where(bin_y == 0, HALF, bin_y)
    special = jnp.logical_and(device == 0, slot == 0)
    bin_x = jnp.where(special, jnp.where(word == 0, HALF, 0), 2 * device + slot)
    top_x, top_y = bin_x == HALF, bin_y == HALF
    wave_x = bin_x.astype(F32) * (2.0 * math.pi / N)
    wave_y = bin_y.astype(F32) * (2.0 * math.pi / N)
    square = wave_x * wave_x + wave_y * wave_y
    anchor = square == 0.0
    norm = jnp.sqrt(jnp.where(anchor, 1.0, square))
    unit_x = jnp.where(anchor, 0.0, wave_x / norm)
    unit_y = jnp.where(anchor, 0.0, wave_y / norm)
    depth = THICKNESS * norm
    series = 1.0 / 5040.0
    for divisor in (-720.0, 120.0, -24.0, 6.0, -2.0, 1.0):
        series = series * depth + 1.0 / divisor
    ratio = jnp.where(depth < 0.25, series, (1.0 - jnp.exp(-depth)) / depth)
    self_z = jnp.where(anchor, 1.0, ratio)
    near = jnp.where(
        anchor, 0.0, 0.5 * depth * ratio * ratio * jnp.exp(-norm * (LAYER_PITCH - THICKNESS))
    )
    step = jnp.exp(-LAYER_PITCH * norm)
    bend = 2.0 * jnp.cos(wave_x) + 2.0 * jnp.cos(wave_y) - 4.0
    scale_x = jnp.where(jnp.logical_or(bin_x == 0, top_x), 1.0, 2.0)
    scale_y = jnp.where(jnp.logical_or(bin_y == 0, top_y), 1.0, 2.0)
    scale = scale_x * scale_y * (1.0 / (N * N))
    return dict(
        x=jnp.where(top_x, 0.0, unit_x),
        y=jnp.where(top_y, 0.0, unit_y),
        top_x=jnp.where(top_x, -unit_x, 0.0),
        top_y=jnp.where(top_y, unit_y, 0.0),
        self_z=self_z,
        near=near,
        step=step,
        bend=bend * scale,
        scale=scale,
    )


def couple_kernel(in_ref, high_ref, low_ref, out_ref, spec_ref, field_ref, keep_ref, top_ref):
    device = lax.axis_index("layer") * LAYERS + lax.axis_index("row")
    low_half = lane_low((8, 128))
    rows = lax.broadcasted_iota(jnp.int32, (8, 128), 0)

    def tile_of(layer, block):
        return in_ref[pl.ds(pl.multiple_of((layer * LAYERS + block) * 8, 8), 8), :]

    def gather(layer, carry):
        for pair in range(4):
            plus, minus = [], []
            for block in (2 * pair, 2 * pair + 1):
                one, two = tile_of(layer, block), tile_of(layer, block + 8)
                plus.append(one + two)
                minus.append(one - two)
            for parity, (one, two) in enumerate((plus, minus)):
                columns = slice(128 * pair, 128 * pair + 128)
                at = pl.ds(pl.multiple_of(layer * 8, 8), 8)
                spec_ref[parity, 0, at, columns] = jnp.where(low_half, one, pltpu.roll(two, 64, 1))
                spec_ref[parity, 1, at, columns] = jnp.where(low_half, pltpu.roll(one, 64, 1), two)
        return carry

    lax.fori_loop(0, LAYERS, gather, 0)
    for parity in range(2):
        waves = product(
            split(spec_ref[parity].reshape(2 * 8 * LAYERS, HALF)),
            (high_ref[parity], low_ref[parity]),
            NT,
        )
        spec_ref[parity] = waves.reshape(2, 8 * LAYERS, HALF)

    def parameter(layer, block, row):
        return jnp.broadcast_to(in_ref[pl.ds((layer * LAYERS + block) * 8 + row, 1), :], (8, 128))

    for parity in range(2):
        for tile in range(2):
            cos_at = slice(128 * tile, 128 * tile + 128)
            sin_at = slice(BINS + 128 * tile, BINS + 128 * tile + 128)
            both = [
                (symbols(device, parity, tile, sine), at)
                for sine, at in ((False, cos_at), (True, sin_at))
            ]

            def load(layer, at):
                at_rows = slice(8 * layer, 8 * layer + 8)
                one, two = spec_ref[parity, 0, at_rows, at], spec_ref[parity, 1, at_rows, at]
                up = jnp.where(rows < 2, pltpu.roll(one, 4, 0), pltpu.roll(two, 6, 0))
                return one, two, up

            (cs, _), (ss, _) = both
            rise = [jnp.zeros((8, 128), F32)] * 2
            for layer in range(LAYERS):
                sat = parameter(layer, 0, 6)
                (xc, yc, zc), (xs, ys, zs) = load(layer, cos_at), load(layer, sin_at)
                along = (cs["x"] * xc + cs["y"] * ys, ss["x"] * xs - ss["y"] * yc)
                for part, (a, z) in enumerate(zip(along, (zc, zs))):
                    sym = both[part][0]
                    a, z = sat * a, sat * z
                    keep_ref[layer, part, 0] = (1.0 - sym["self_z"]) * a + rise[part]
                    keep_ref[layer, part, 1] = sym["self_z"] * z + rise[part]
                    keep_ref[layer, part, 2] = sym["near"] * (a - z)
                    rise[part] = sym["step"] * rise[part] + sym["near"] * (a + z)
            fall = [jnp.zeros((8, 128), F32)] * 2
            for layer in reversed(range(LAYERS)):
                psi, chi = [], []
                for part in range(2):
                    sym = both[part][0]
                    psi.append(keep_ref[layer, part, 0] + fall[part])
                    chi.append(keep_ref[layer, part, 1] - fall[part])
                    fall[part] = sym["step"] * fall[part] + keep_ref[layer, part, 2]
                stiff = parameter(layer, 0, 7)
                below = RKKY_STRENGTH * parameter(layer, 1, 6) if layer > 0 else None
                above = RKKY_STRENGTH * parameter(layer, 1, 7) if layer < LAYERS - 1 else None
                for part, (sym, at) in enumerate(both):
                    here = load(layer, at)
                    cross = cs["y"] * psi[1] if part == 0 else -ss["y"] * psi[0]
                    field = [-sym["x"] * psi[part], cross, -chi[part]]
                    pair = [0.0, 0.0, 0.0]
                    if below is not None:
                        pair = [p + below * v for p, v in zip(pair, load(layer - 1, at))]
                    if above is not None:
                        pair = [p + above * v for p, v in zip(pair, load(layer + 1, at))]
                    hx, hy, hz = (
                        sym["scale"] * (f + p) + (stiff * sym["bend"]) * v
                        for f, p, v in zip(field, pair, here)
                    )
                    at_rows = slice(8 * layer, 8 * layer + 8)
                    field_ref[parity, 0, at_rows, at] = jnp.where(rows < 4, hx, pltpu.roll(hz, 4, 0))
                    field_ref[parity, 1, at_rows, at] = jnp.where(rows < 4, hy, pltpu.roll(hz, 2, 0))

            def top():
                for part, (sym, at) in enumerate(both):
                    rise = jnp.zeros((8, 128), F32)
                    fall = rise
                    for layer in range(LAYERS):
                        sat = parameter(layer, 0, 6)
                        x, y, _ = load(layer, at)
                        e = sat * (sym["top_x"] * x + sym["top_y"] * y)
                        top_ref[layer, 0] = (1.0 - sym["self_z"]) * e + rise
                        top_ref[layer, 1] = sym["near"] * e
                        rise = sym["step"] * rise + sym["near"] * e
                    for layer in reversed(range(LAYERS)):
                        psi = sym["scale"] * (top_ref[layer, 0] + fall)
                        fall = sym["step"] * fall + top_ref[layer, 1]
                        at_rows = slice(8 * layer, 8 * layer + 8)
                        for half, key in enumerate(("top_x", "top_y")):
                            field_ref[parity, half, at_rows, at] -= jnp.where(
                                rows < 4, sym[key] * psi, 0.0
                            )

            if parity == 0 and tile == 0:
                top()
            else:
                pl.when(device == 0)(top)

    for parity in range(2):
        spec_ref[parity] = product(
            split(field_ref[parity].reshape(2 * 8 * LAYERS, HALF)),
            (high_ref[parity], low_ref[parity]),
            NN,
        ).reshape(2, 8 * LAYERS, HALF)

    def scatter(layer, carry):
        at = pl.ds(pl.multiple_of(layer * 8, 8), 8)
        for pair in range(4):
            columns = slice(128 * pair, 128 * pair + 128)
            even = [spec_ref[0, half, at, columns] for half in range(2)]
            odd = [spec_ref[1, half, at, columns] for half in range(2)]
            for far in range(2):
                one, two = (e - o if far else e + o for e, o in zip(even, odd))
                block = layer * LAYERS + 8 * far + 2 * pair
                out_ref[pl.ds(pl.multiple_of(block * 8, 8), 8), :] = jnp.where(
                    low_half, one, pltpu.roll(two, 64, 1)
                )
                out_ref[pl.ds(pl.multiple_of(block * 8 + 8, 8), 8), :] = jnp.where(
                    low_half, pltpu.roll(one, 64, 1), two
                )
        return carry

    lax.fori_loop(0, LAYERS, scatter, 0)


def torque_kernel(damping_ref, magnet_ref, in_ref, high_ref, low_ref, out_ref):
    low_half = lane_low((DEVICES, 128))
    first = lax.broadcasted_iota(jnp.int32, (DEVICES, 128), 0) == 0
    parts = []
    for slot in range(2):
        one = in_ref[pl.ds(slot, DEVICES, stride=8), :]
        two = in_ref[pl.ds(2 + slot, DEVICES, stride=8), :]
        up = in_ref[pl.ds(4 + slot, DEVICES, stride=8), :]
        if slot == 0:
            x_one, x_two = jnp.where(first, two, one), jnp.where(first, one, two)
        else:
            x_one, x_two = one, two
        cosine = jnp.concatenate(
            [jnp.where(low_half, x_one, two), pltpu.roll(up, 64, 1)], axis=1
        )
        sine = jnp.concatenate([jnp.where(low_half, x_two, -one), -up], axis=1)
        waves = jnp.concatenate([cosine, sine], axis=0)
        parts.append(product(split(waves), (high_ref[slot], low_ref[slot]), TN))
    damping = damping_ref[0]
    factor = -1.0 / (1.0 + damping * damping)
    for far in range(2):
        at = slice(HALF * far, HALF * far + HALF)
        field = parts[0] - parts[1] if far else parts[0] + parts[1]
        h = [field[ROWS * c : ROWS * c + ROWS] for c in range(3)]
        m = [magnet_ref[ROWS * c : ROWS * c + ROWS, at] for c in range(3)]
        p = [m[c - 2] * h[c - 1] - m[c - 1] * h[c - 2] for c in range(3)]
        for c in range(3):
            relax = m[c - 2] * p[c - 1] - m[c - 1] * p[c - 2]
            out_ref[ROWS * c : ROWS * c + ROWS, at] = factor * (p[c] + damping * relax)


def call(kernel, out, scratch, inputs, smem):
    spaces = [pltpu.SMEM] * smem + [pltpu.VMEM] * (len(inputs) - smem)
    return pl.pallas_call(
        kernel,
        out_shape=jax.ShapeDtypeStruct(out, F32),
        in_specs=[pl.BlockSpec(memory_space=space) for space in spaces],
        out_specs=pl.BlockSpec(memory_space=pltpu.VMEM),
        scratch_shapes=[pltpu.VMEM(shape, F32) for shape in scratch],
    )(*inputs)


def exchange(blocks):
    blocks = blocks.reshape(DEVICES, 8, 128)
    blocks = lax.all_to_all(blocks, ("layer", "row"), split_axis=0, concat_axis=0, tiled=True)
    return blocks.reshape(8 * DEVICES, 128)


def on_device(magnet, saturation, stiffness, damping, interface_sign):
    flat = magnet.reshape(3 * ROWS, N)
    high, low = wave_tables()
    buffer = (8 * DEVICES, 128)
    waves = call(
        forward_x_kernel, buffer, [], (saturation, stiffness, interface_sign, flat, high, low), 3
    )
    spectrum = (2, 2, 8 * LAYERS, HALF)
    fields = call(
        couple_kernel,
        buffer,
        [spectrum, spectrum, (LAYERS, 2, 3, 8, 128), (LAYERS, 2, 8, 128)],
        (exchange(waves), high, low),
        0,
    )
    torque = call(
        torque_kernel, flat.shape, [], (damping, flat, exchange(fields), high, low), 1
    )
    return torque.reshape(magnet.shape)


def solution(mesh):
    in_specs = (P(None, "layer", "row", None), P("layer"), P("layer"), P("layer"), P("layer", None))
    out_specs = P(None, "layer", "row", None)
    return jax.shard_map(
        on_device, mesh=mesh, in_specs=in_specs, out_specs=out_specs, check_vma=False
    )
```

```python
import functools
import math

import jax
import jax.numpy as jnp
import numpy as np
from jax import lax
from jax.experimental import pallas as pl
from jax.experimental.pallas import tpu as pltpu
from jax.sharding import PartitionSpec as P

N = 1024
HALF = N // 2
BINS = N // 4
LAYERS = 16
ROWS = 64
DEVICES = 256
THICKNESS = 1.0
LAYER_PITCH = 1.5
RKKY_STRENGTH = 0.8
F32 = jnp.float32
BF16 = jnp.bfloat16
NT = (((1,), (1,)), ((), ()))
NN = (((1,), (0,)), ((), ()))
TN = (((0,), (0,)), ((), ()))
USED = 6
MESH = pl.DeviceIdType.MESH


def wave_tables():
    grid = np.arange(HALF)
    bins = np.arange(BINS)
    tables = []
    for parity in range(2):
        phase = (2 * bins[:, None] + parity) * grid[None, :] % N * (2.0 * np.pi / N)
        cosines, sines = np.cos(phase), np.sin(phase)
        if parity == 0:
            sines[0] = 1.0 - 2.0 * (grid % 2)
        tables.append(np.concatenate([cosines, sines], axis=0))
    exact = np.stack(tables)
    high = exact.astype(np.dtype(BF16))
    low = (exact - high.astype(np.float64)).astype(np.dtype(BF16))
    return jnp.asarray(high), jnp.asarray(low)


def split(value):
    high = value.astype(BF16)
    return high, (value - high.astype(F32)).astype(BF16)


def product(left, right, dims):
    (left_high, left_low), (right_high, right_low) = left, right
    dot = functools.partial(lax.dot_general, dimension_numbers=dims, preferred_element_type=F32)
    return dot(left_high, right_high) + (dot(left_high, right_low) + dot(left_low, right_high))


def lane_low(shape):
    return lax.broadcasted_iota(jnp.int32, shape, len(shape) - 1) < ROWS


def forward_x(magnet_ref, high_ref, low_ref, out_ref, slot):
    left, right = magnet_ref[:, :HALF], magnet_ref[:, HALF:]
    low_half = lane_low((DEVICES, 128))
    folded = left - right if slot else left + right
    folded = jnp.concatenate([folded, folded[2 * ROWS :]], axis=0)
    waves = product((high_ref[slot], low_ref[slot]), split(folded), NT)
    cosine, sine = waves[:BINS], waves[BINS:]
    one, two = cosine[:, :128], sine[:, :128]
    if slot == 0:
        first = lax.broadcasted_iota(jnp.int32, (DEVICES, 128), 0) == 0
        x_one, x_two = jnp.where(first, two, one), jnp.where(first, one, two)
    else:
        x_one, x_two = one, two
    out_ref[pl.ds(slot, DEVICES, stride=8), :] = jnp.where(low_half, x_one, -two)
    out_ref[pl.ds(2 + slot, DEVICES, stride=8), :] = jnp.where(low_half, x_two, one)
    out_ref[pl.ds(4 + slot, DEVICES, stride=8), :] = jnp.where(
        low_half, -sine[:, 128:], cosine[:, 128:]
    )


def symbols(device, parity, tile, sine):
    shape = (8, 128)
    row = lax.broadcasted_iota(jnp.int32, shape, 0)
    slot, word = row % 2, row // 2 % 2
    bin_y = 2 * (lax.broadcasted_iota(jnp.int32, shape, 1) + 128 * tile) + parity
    if sine and parity == 0:
        bin_y = jnp.where(bin_y == 0, HALF, bin_y)
    special = jnp.logical_and(device == 0, slot == 0)
    bin_x = jnp.where(special, jnp.where(word == 0, HALF, 0), 2 * device + slot)
    top_x, top_y = bin_x == HALF, bin_y == HALF
    wave_x = bin_x.astype(F32) * (2.0 * math.pi / N)
    wave_y = bin_y.astype(F32) * (2.0 * math.pi / N)
    square = wave_x * wave_x + wave_y * wave_y
    anchor = square == 0.0
    norm = jnp.sqrt(jnp.where(anchor, 1.0, square))
    unit_x = jnp.where(anchor, 0.0, wave_x / norm)
    unit_y = jnp.where(anchor, 0.0, wave_y / norm)
    depth = THICKNESS * norm
    series = 1.0 / 5040.0
    for divisor in (-720.0, 120.0, -24.0, 6.0, -2.0, 1.0):
        series = series * depth + 1.0 / divisor
    ratio = jnp.where(depth < 0.25, series, (1.0 - jnp.exp(-depth)) / depth)
    self_z = jnp.where(anchor, 1.0, ratio)
    near = jnp.where(
        anchor, 0.0, 0.5 * depth * ratio * ratio * jnp.exp(-norm * (LAYER_PITCH - THICKNESS))
    )
    step = jnp.exp(-LAYER_PITCH * norm)
    bend = 2.0 * jnp.cos(wave_x) + 2.0 * jnp.cos(wave_y) - 4.0
    scale_x = jnp.where(jnp.logical_or(bin_x == 0, top_x), 1.0, 2.0)
    scale_y = jnp.where(jnp.logical_or(bin_y == 0, top_y), 1.0, 2.0)
    scale = scale_x * scale_y * (1.0 / (N * N))
    return dict(
        x=jnp.where(top_x, 0.0, unit_x),
        y=jnp.where(top_y, 0.0, unit_y),
        top_x=jnp.where(top_x, -unit_x, 0.0),
        top_y=jnp.where(top_y, unit_y, 0.0),
        self_z=self_z,
        near=near,
        step=step,
        bend=bend * scale,
        scale=scale,
    )


def couple(in_ref, high_ref, low_ref, out_ref, trait_ref, spec_ref, field_ref, keep_ref, top_ref):
    device = lax.axis_index("layer") * LAYERS + lax.axis_index("row")
    low_half = lane_low((8, 128))
    rows = lax.broadcasted_iota(jnp.int32, (8, 128), 0)

    def tile_of(layer, block):
        return in_ref[pl.ds(pl.multiple_of((layer * LAYERS + block) * 8, 8), 8), :]

    def gather(layer, carry):
        for pair in range(4):
            plus, minus = [], []
            for block in (2 * pair, 2 * pair + 1):
                one, two = tile_of(layer, block), tile_of(layer, block + 8)
                plus.append(one + two)
                minus.append(one - two)
            for parity, (one, two) in enumerate((plus, minus)):
                columns = slice(128 * pair, 128 * pair + 128)
                at = pl.ds(pl.multiple_of(layer * 8, 8), 8)
                spec_ref[parity, 0, at, columns] = jnp.where(low_half, one, pltpu.roll(two, 64, 1))
                spec_ref[parity, 1, at, columns] = jnp.where(low_half, pltpu.roll(one, 64, 1), two)
        return carry

    lax.fori_loop(0, LAYERS, gather, 0)
    for parity in range(2):
        waves = product(
            split(spec_ref[parity].reshape(2 * 8 * LAYERS, HALF)),
            (high_ref[parity], low_ref[parity]),
            NT,
        )
        spec_ref[parity] = waves.reshape(2, 8 * LAYERS, HALF)

    def trait(layer, row):
        return jnp.broadcast_to(trait_ref[8 * layer + row : 8 * layer + row + 1, :], (8, 128))

    for parity in range(2):
        for tile in range(2):
            cos_at = slice(128 * tile, 128 * tile + 128)
            sin_at = slice(BINS + 128 * tile, BINS + 128 * tile + 128)
            both = [
                (symbols(device, parity, tile, sine), at)
                for sine, at in ((False, cos_at), (True, sin_at))
            ]

            def load(layer, at):
                at_rows = slice(8 * layer, 8 * layer + 8)
                one, two = spec_ref[parity, 0, at_rows, at], spec_ref[parity, 1, at_rows, at]
                up = jnp.where(rows < 2, pltpu.roll(one, 4, 0), pltpu.roll(two, 6, 0))
                return one, two, up

            (cs, _), (ss, _) = both
            rise = [jnp.zeros((8, 128), F32)] * 2
            for layer in range(LAYERS):
                sat = trait(layer, 0)
                (xc, yc, zc), (xs, ys, zs) = load(layer, cos_at), load(layer, sin_at)
                along = (cs["x"] * xc + cs["y"] * ys, ss["x"] * xs - ss["y"] * yc)
                for part, (a, z) in enumerate(zip(along, (zc, zs))):
                    sym = both[part][0]
                    a, z = sat * a, sat * z
                    keep_ref[layer, part, 0] = (1.0 - sym["self_z"]) * a + rise[part]
                    keep_ref[layer, part, 1] = sym["self_z"] * z + rise[part]
                    keep_ref[layer, part, 2] = sym["near"] * (a - z)
                    rise[part] = sym["step"] * rise[part] + sym["near"] * (a + z)
            fall = [jnp.zeros((8, 128), F32)] * 2
            for layer in reversed(range(LAYERS)):
                psi, chi = [], []
                for part in range(2):
                    sym = both[part][0]
                    psi.append(keep_ref[layer, part, 0] + fall[part])
                    chi.append(keep_ref[layer, part, 1] - fall[part])
                    fall[part] = sym["step"] * fall[part] + keep_ref[layer, part, 2]
                stiff = trait(layer, 1)
                below = RKKY_STRENGTH * trait(layer, 2) if layer > 0 else None
                above = RKKY_STRENGTH * trait(layer, 3) if layer < LAYERS - 1 else None
                for part, (sym, at) in enumerate(both):
                    here = load(layer, at)
                    cross = cs["y"] * psi[1] if part == 0 else -ss["y"] * psi[0]
                    field = [-sym["x"] * psi[part], cross, -chi[part]]
                    pair = [0.0, 0.0, 0.0]
                    if below is not None:
                        pair = [p + below * v for p, v in zip(pair, load(layer - 1, at))]
                    if above is not None:
                        pair = [p + above * v for p, v in zip(pair, load(layer + 1, at))]
                    hx, hy, hz = (
                        sym["scale"] * (f + p) + (stiff * sym["bend"]) * v
                        for f, p, v in zip(field, pair, here)
                    )
                    at_rows = slice(8 * layer, 8 * layer + 8)
                    field_ref[parity, 0, at_rows, at] = jnp.where(rows < 4, hx, pltpu.roll(hz, 4, 0))
                    field_ref[parity, 1, at_rows, at] = jnp.where(rows < 4, hy, pltpu.roll(hz, 2, 0))

            def top():
                for part, (sym, at) in enumerate(both):
                    rise = jnp.zeros((8, 128), F32)
                    fall = rise
                    for layer in range(LAYERS):
                        sat = trait(layer, 0)
                        x, y, _ = load(layer, at)
                        e = sat * (sym["top_x"] * x + sym["top_y"] * y)
                        top_ref[layer, 0] = (1.0 - sym["self_z"]) * e + rise
                        top_ref[layer, 1] = sym["near"] * e
                        rise = sym["step"] * rise + sym["near"] * e
                    for layer in reversed(range(LAYERS)):
                        psi = sym["scale"] * (top_ref[layer, 0] + fall)
                        fall = sym["step"] * fall + top_ref[layer, 1]
                        at_rows = slice(8 * layer, 8 * layer + 8)
                        for half, key in enumerate(("top_x", "top_y")):
                            field_ref[parity, half, at_rows, at] -= jnp.where(
                                rows < 4, sym[key] * psi, 0.0
                            )

            if parity == 0 and tile == 0:
                top()
            else:
                pl.when(device == 0)(top)

    for parity in range(2):
        spec_ref[parity] = product(
            split(field_ref[parity].reshape(2 * 8 * LAYERS, HALF)),
            (high_ref[parity], low_ref[parity]),
            NN,
        ).reshape(2, 8 * LAYERS, HALF)

    def scatter(layer, carry):
        at = pl.ds(pl.multiple_of(layer * 8, 8), 8)
        for pair in range(4):
            columns = slice(128 * pair, 128 * pair + 128)
            even = [spec_ref[0, half, at, columns] for half in range(2)]
            odd = [spec_ref[1, half, at, columns] for half in range(2)]
            for far in range(2):
                one, two = (e - o if far else e + o for e, o in zip(even, odd))
                block = layer * LAYERS + 8 * far + 2 * pair
                out_ref[pl.ds(pl.multiple_of(block * 8, 8), 8), :] = jnp.where(
                    low_half, one, pltpu.roll(two, 64, 1)
                )
                out_ref[pl.ds(pl.multiple_of(block * 8 + 8, 8), 8), :] = jnp.where(
                    low_half, pltpu.roll(one, 64, 1), two
                )
        return carry

    lax.fori_loop(0, LAYERS, scatter, 0)


def finish(damping, magnet_ref, in_ref, high_ref, low_ref, out_ref):
    low_half = lane_low((DEVICES, 128))
    first = lax.broadcasted_iota(jnp.int32, (DEVICES, 128), 0) == 0
    parts = []
    for slot in range(2):
        one = in_ref[pl.ds(slot, DEVICES, stride=8), :]
        two = in_ref[pl.ds(2 + slot, DEVICES, stride=8), :]
        up = in_ref[pl.ds(4 + slot, DEVICES, stride=8), :]
        if slot == 0:
            x_one, x_two = jnp.where(first, two, one), jnp.where(first, one, two)
        else:
            x_one, x_two = one, two
        cosine = jnp.concatenate(
            [jnp.where(low_half, x_one, two), pltpu.roll(up, 64, 1)], axis=1
        )
        sine = jnp.concatenate([jnp.where(low_half, x_two, -one), -up], axis=1)
        waves = jnp.concatenate([cosine, sine], axis=0)
        parts.append(product(split(waves), (high_ref[slot], low_ref[slot]), TN))
    factor = -1.0 / (1.0 + damping * damping)
    for far in range(2):
        at = slice(HALF * far, HALF * far + HALF)
        field = parts[0] - parts[1] if far else parts[0] + parts[1]
        h = [field[ROWS * c : ROWS * c + ROWS] for c in range(3)]
        m = [magnet_ref[ROWS * c : ROWS * c + ROWS, at] for c in range(3)]
        p = [m[c - 2] * h[c - 1] - m[c - 1] * h[c - 2] for c in range(3)]
        for c in range(3):
            relax = m[c - 2] * p[c - 1] - m[c - 1] * p[c - 2]
            out_ref[ROWS * c : ROWS * c + ROWS, at] = factor * (p[c] + damping * relax)


def kernel(
    sat_ref,
    stiff_ref,
    damping_ref,
    sign_ref,
    magnet_ref,
    high_ref,
    low_ref,
    out_ref,
    send_one,
    recv_one,
    send_two,
    recv_two,
    trait_ref,
    spec_ref,
    field_ref,
    keep_ref,
    top_ref,
    send_sems,
    recv_sems,
    ready,
):
    layer, row = lax.axis_index("layer"), lax.axis_index("row")
    me = layer * LAYERS + row

    def turned(index, by):
        return jnp.bitwise_and(index + by, LAYERS - 1)

    barrier = pltpu.get_barrier_semaphore()

    def greet(step, carry):
        for target in ((layer, turned(row, step)), (turned(layer, step), row)):
            pl.semaphore_signal(barrier, inc=1, device_id=target, device_id_type=MESH)
        return carry

    lax.fori_loop(1, LAYERS, greet, 0)
    kinds = lax.broadcasted_iota(jnp.int32, (8, 128), 0)
    traits = jnp.where(kinds == 0, sat_ref[0], stiff_ref[0])
    traits = jnp.where(kinds == 2, sign_ref[0, 0].astype(F32), traits)
    traits = jnp.where(kinds == 3, sign_ref[0, 1].astype(F32), traits)
    own_trait = pl.ds(pl.multiple_of(8 * layer, 8), 8)
    trait_ref[own_trait, :] = traits
    forward_x(magnet_ref, high_ref, low_ref, send_one, 0)
    pl.semaphore_wait(barrier, 2 * (LAYERS - 1))

    def vouch(step, carry):
        target = (layer, turned(row, step))
        pl.semaphore_signal(ready, inc=1, device_id=target, device_id_type=MESH)
        return carry

    lax.fori_loop(1, LAYERS, vouch, 0)
    forward_x(magnet_ref, high_ref, low_ref, send_one, 1)
    pl.semaphore_wait(ready, LAYERS - 1)

    def tell(step, carry):
        pltpu.make_async_remote_copy(
            src_ref=trait_ref.at[own_trait],
            dst_ref=trait_ref.at[own_trait],
            send_sem=send_sems.at[2],
            recv_sem=recv_sems.at[2],
            device_id=(turned(layer, step), row),
            device_id_type=MESH,
        ).start()
        return carry

    lax.fori_loop(1, LAYERS, tell, 0)

    def exchange(source, target, index):
        def push(step, carry):
            other = jnp.bitwise_and(me + step, DEVICES - 1)
            pltpu.make_async_remote_copy(
                src_ref=source.at[pl.ds(pl.multiple_of(8 * other, 8), USED)],
                dst_ref=target.at[pl.ds(pl.multiple_of(8 * me, 8), USED)],
                send_sem=send_sems.at[index],
                recv_sem=recv_sems.at[index],
                device_id=(jnp.right_shift(other, 4), jnp.bitwise_and(other, LAYERS - 1)),
                device_id_type=MESH,
            ).start()
            return carry

        lax.fori_loop(1, DEVICES, push, 0)
        mine = pl.ds(pl.multiple_of(8 * me, 8), 8)
        target[mine, :] = source[mine, :]
        drain(source, target, index, USED * (DEVICES - 1))

    def drain(source, target, index, count):
        every = pl.ds(0, count)
        pltpu.make_async_copy(source.at[every], source.at[every], send_sems.at[index]).wait()
        pltpu.make_async_copy(target.at[every], target.at[every], recv_sems.at[index]).wait()

    exchange(send_one, recv_one, 0)
    drain(trait_ref, trait_ref, 2, 8 * (LAYERS - 1))
    couple(
        recv_one, high_ref, low_ref, send_two, trait_ref, spec_ref, field_ref, keep_ref, top_ref
    )
    exchange(send_two, recv_two, 1)
    finish(damping_ref[0], magnet_ref, recv_two, high_ref, low_ref, out_ref)


def on_device(magnet, saturation, stiffness, damping, interface_sign):
    flat = magnet.reshape(3 * ROWS, N)
    spaces = [pltpu.SMEM] * 4 + [pltpu.VMEM] * 3
    buffer, spectrum = (8 * DEVICES, 128), (2, 2, 8 * LAYERS, HALF)
    shapes = [buffer] * 4 + [(8 * LAYERS, 128), spectrum, spectrum]
    shapes += [(LAYERS, 2, 3, 8, 128), (LAYERS, 2, 8, 128)]
    torque = pl.pallas_call(
        kernel,
        out_shape=jax.ShapeDtypeStruct(flat.shape, F32),
        in_specs=[pl.BlockSpec(memory_space=space) for space in spaces],
        out_specs=pl.BlockSpec(memory_space=pltpu.VMEM),
        scratch_shapes=[pltpu.VMEM(shape, F32) for shape in shapes]
        + [pltpu.SemaphoreType.DMA((3,))] * 2
        + [pltpu.SemaphoreType.REGULAR],
        compiler_params=pltpu.CompilerParams(collective_id=0, has_side_effects=True),
        name="torque",
    )(saturation, stiffness, damping, interface_sign, flat, *wave_tables())
    return torque.reshape(magnet.shape)


def solution(mesh):
    in_specs = (P(None, "layer", "row", None), P("layer"), P("layer"), P("layer"), P("layer", None))
    out_specs = P(None, "layer", "row", None)
    return jax.shard_map(
        on_device, mesh=mesh, in_specs=in_specs, out_specs=out_specs, check_vma=False
    )
```

```python
import functools
import math

import jax
import jax.numpy as jnp
import numpy as np
from jax import lax
from jax.experimental import pallas as pl
from jax.experimental.pallas import tpu as pltpu
from jax.sharding import PartitionSpec as P

N = 1024
HALF = N // 2
BINS = N // 4
LAYERS = 16
ROWS = 64
DEVICES = 256
THICKNESS = 1.0
LAYER_PITCH = 1.5
RKKY_STRENGTH = 0.8
F32 = jnp.float32
BF16 = jnp.bfloat16
NT = (((1,), (1,)), ((), ()))
NN = (((1,), (0,)), ((), ()))
TN = (((0,), (0,)), ((), ()))
USED = 3
PAIRS = LAYERS // 2
BLOCKS = DEVICES // 2
TILE = (8, 128)
MESH = pl.DeviceIdType.MESH


def wave_tables():
    grid = np.arange(HALF)
    bins = np.arange(BINS)
    tables = []
    for parity in range(2):
        phase = (2 * bins[:, None] + parity) * grid[None, :] % N * (2.0 * np.pi / N)
        cosines, sines = np.cos(phase), np.sin(phase)
        if parity == 0:
            sines[0] = 1.0 - 2.0 * (grid % 2)
        tables.append(np.concatenate([cosines, sines], axis=0))
    exact = np.stack(tables)
    high = exact.astype(np.dtype(BF16))
    low = (exact - high.astype(np.float64)).astype(np.dtype(BF16))
    return jnp.asarray(high), jnp.asarray(low)


def split(value):
    high = value.astype(BF16)
    return high, (value - high.astype(F32)).astype(BF16)


def product(left, right, dims):
    (left_high, left_low), (right_high, right_low) = left, right
    dot = functools.partial(lax.dot_general, dimension_numbers=dims, preferred_element_type=F32)
    return dot(left_high, right_high) + (dot(left_high, right_low) + dot(left_low, right_high))


def lane_low(shape):
    return lax.broadcasted_iota(jnp.int32, shape, len(shape) - 1) < ROWS


def flat(ref):
    return ref.reshape(ref.shape[0] * 8, 128)


def forward_x(magnet_ref, high_ref, low_ref, out_ref, slot):
    left, right = magnet_ref[:, :HALF], magnet_ref[:, HALF:]
    low_half = lane_low((DEVICES, 128))
    folded = left - right if slot else left + right
    folded = jnp.concatenate([folded, folded[2 * ROWS :]], axis=0)
    waves = product((high_ref[slot], low_ref[slot]), split(folded), NT)
    cosine, sine = waves[:BINS], waves[BINS:]
    one, two = cosine[:, :128], sine[:, :128]
    if slot == 0:
        first = lax.broadcasted_iota(jnp.int32, (DEVICES, 128), 0) == 0
        x_one, x_two = jnp.where(first, two, one), jnp.where(first, one, two)
    else:
        x_one, x_two = one, two
    out = flat(out_ref)
    out[pl.ds(4 * slot, DEVICES, stride=8), :] = jnp.where(low_half, x_one, -two)
    out[pl.ds(4 * slot + 1, DEVICES, stride=8), :] = jnp.where(low_half, x_two, one)
    out[pl.ds(4 * slot + 2, DEVICES, stride=8), :] = jnp.where(
        low_half, -sine[:, 128:], cosine[:, 128:]
    )


def symbols(device, slot, parity, tile, sine):
    bin_y = 2 * (lax.broadcasted_iota(jnp.int32, TILE, 1) + 128 * tile) + parity
    if sine and parity == 0:
        bin_y = jnp.where(bin_y == 0, HALF, bin_y)
    bin_x = jnp.full(TILE, 2 * device + slot, jnp.int32)
    if slot == 0:
        word = lax.broadcasted_iota(jnp.int32, TILE, 0) % 2
        bin_x = jnp.where(device == 0, jnp.where(word == 0, HALF, 0), bin_x)
    top_x, top_y = bin_x == HALF, bin_y == HALF
    wave_x = bin_x.astype(F32) * (2.0 * math.pi / N)
    wave_y = bin_y.astype(F32) * (2.0 * math.pi / N)
    square = wave_x * wave_x + wave_y * wave_y
    anchor = square == 0.0
    norm = jnp.sqrt(jnp.where(anchor, 1.0, square))
    unit_x = jnp.where(anchor, 0.0, wave_x / norm)
    unit_y = jnp.where(anchor, 0.0, wave_y / norm)
    depth = THICKNESS * norm
    series = 1.0 / 5040.0
    for divisor in (-720.0, 120.0, -24.0, 6.0, -2.0, 1.0):
        series = series * depth + 1.0 / divisor
    ratio = jnp.where(depth < 0.25, series, (1.0 - jnp.exp(-depth)) / depth)
    self_z = jnp.where(anchor, 1.0, ratio)
    near = jnp.where(
        anchor, 0.0, 0.5 * depth * ratio * ratio * jnp.exp(-norm * (LAYER_PITCH - THICKNESS))
    )
    step = jnp.exp(-LAYER_PITCH * norm)
    bend = 2.0 * jnp.cos(wave_x) + 2.0 * jnp.cos(wave_y) - 4.0
    scale_x = jnp.where(jnp.logical_or(bin_x == 0, top_x), 1.0, 2.0)
    scale_y = jnp.where(jnp.logical_or(bin_y == 0, top_y), 1.0, 2.0)
    scale = scale_x * scale_y * (1.0 / (N * N))
    return dict(
        x=jnp.where(top_x, 0.0, unit_x),
        y=jnp.where(top_y, 0.0, unit_y),
        top_x=jnp.where(top_x, -unit_x, 0.0),
        top_y=jnp.where(top_y, unit_y, 0.0),
        self_z=self_z,
        near=near,
        step=step,
        double=step * step,
        bend=bend * scale,
        scale=scale,
    )


def pack_traits(trait_ref, pack_ref):
    low_rows = lax.broadcasted_iota(jnp.int32, TILE, 0) < 4
    for pair in range(PAIRS):
        for kind in range(4):
            low, high = (
                jnp.broadcast_to(trait_ref[layer, kind : kind + 1, :], TILE)
                for layer in (2 * pair, 2 * pair + 1)
            )
            if kind == 2 and pair == 0:
                low = jnp.zeros(TILE, F32)
            if kind == 3 and pair == PAIRS - 1:
                high = jnp.zeros(TILE, F32)
            value = jnp.where(low_rows, low, high)
            pack_ref[kind, pair] = RKKY_STRENGTH * value if kind > 1 else value


def couple(slot, in_ref, high_ref, low_ref, out_ref, pack_ref, spec_ref, field_ref, keep_ref):
    device = lax.axis_index("layer") * LAYERS + lax.axis_index("row")
    low_half = lane_low(TILE)
    rows = lax.broadcasted_iota(jnp.int32, TILE, 0)
    low_rows = rows < 4
    place = jnp.bitwise_and(rows, 3)
    zero = jnp.zeros(TILE, F32)

    def gather(pair, carry):
        at = pl.ds(pl.multiple_of(pair * 8, 8), 8)
        for group in range(4):
            plus, minus = [], []
            for block in (2 * group, 2 * group + 1):
                first = slot * BLOCKS + pair * LAYERS + block
                one, two = in_ref[first], in_ref[first + 8]
                plus.append(one + two)
                minus.append(one - two)
            for parity, (one, two) in enumerate((plus, minus)):
                columns = slice(128 * group, 128 * group + 128)
                spec_ref[parity, 0, at, columns] = jnp.where(low_half, one, pltpu.roll(two, 64, 1))
                spec_ref[parity, 1, at, columns] = jnp.where(low_half, pltpu.roll(one, 64, 1), two)
        return carry

    lax.fori_loop(0, PAIRS, gather, 0, unroll=2)
    for parity in range(2):
        waves = product(
            split(spec_ref[parity].reshape(2 * 8 * PAIRS, HALF)),
            (high_ref[parity], low_ref[parity]),
            NT,
        )
        spec_ref[parity] = waves.reshape(2, 8 * PAIRS, HALF)

    def turn(value):
        return pltpu.roll(value, 4, 0)

    for parity in range(2):
        for tile in range(2):
            both = [
                (
                    symbols(device, slot, parity, tile, sine),
                    slice(BINS * sine + 128 * tile, BINS * sine + 128 * tile + 128),
                )
                for sine in range(2)
            ]

            def load(pair, at):
                at_rows = slice(8 * pair, 8 * pair + 8)
                one, two = spec_ref[parity, 0, at_rows, at], spec_ref[parity, 1, at_rows, at]
                up = jnp.where(place == 0, pltpu.roll(one, 6, 0), pltpu.roll(two, 7, 0))
                return one, two, up

            (cs, cos_at), (ss, sin_at) = both
            rise, last = [zero, zero], [zero, zero]
            for pair in range(PAIRS):
                sat = pack_ref[0, pair]
                (xc, yc, zc), (xs, ys, zs) = load(pair, cos_at), load(pair, sin_at)
                along = (cs["x"] * xc + cs["y"] * ys, ss["x"] * xs - ss["y"] * yc)
                for part, (a, z) in enumerate(zip(along, (zc, zs))):
                    sym = both[part][0]
                    keep_ref[pair, part, 3] = z
                    a, z = sat * a, sat * z
                    up, down = sym["near"] * (a + z), sym["near"] * (a - z)
                    turned = turn(up)
                    if pair:
                        rise[part] = rise[part] + jnp.where(low_rows, 0.0, turned)
                    else:
                        rise[part] = jnp.where(low_rows, 0.0, turned)
                    keep_ref[pair, part, 0] = (1.0 - sym["self_z"]) * a + rise[part]
                    keep_ref[pair, part, 1] = sym["self_z"] * z + rise[part]
                    keep_ref[pair, part, 2] = down
                    rise[part] = (
                        sym["double"] * rise[part]
                        + sym["step"] * up
                        + jnp.where(low_rows, turned, 0.0)
                    )
            fall = [zero, zero]
            for pair in reversed(range(PAIRS)):
                psi, chi = [], []
                for part in range(2):
                    sym = both[part][0]
                    down = keep_ref[pair, part, 2]
                    turned = turn(down)
                    fall[part] = fall[part] + jnp.where(low_rows, turned, 0.0)
                    psi.append(keep_ref[pair, part, 0] + fall[part])
                    chi.append(keep_ref[pair, part, 1] - fall[part])
                    fall[part] = (
                        sym["double"] * fall[part]
                        + sym["step"] * down
                        + jnp.where(low_rows, 0.0, turned)
                    )
                stiff, below, above = (pack_ref[kind, pair] for kind in (1, 2, 3))
                at_rows = slice(8 * pair, 8 * pair + 8)

                def raw(which, part, at):
                    rows_of = slice(8 * which, 8 * which + 8)
                    one, two = (spec_ref[parity, half, rows_of, at] for half in range(2))
                    return one, two, keep_ref[which, part, 3]

                for part, (sym, at) in enumerate(both):
                    here = raw(pair, part, at)
                    before = raw(pair - 1, part, at) if pair else (zero,) * 3
                    after = raw(pair + 1, part, at) if pair < PAIRS - 1 else (zero,) * 3
                    cross = cs["y"] * psi[1] if part == 0 else -ss["y"] * psi[0]
                    field = (-sym["x"] * psi[part], cross, -chi[part])
                    hx, hy, hz = (
                        sym["scale"]
                        * (
                            f
                            + below * turn(jnp.where(low_rows, v, b))
                            + above * turn(jnp.where(low_rows, n, v))
                        )
                        + (stiff * sym["bend"]) * v
                        for f, v, b, n in zip(field, here, before, after)
                    )
                    field_ref[parity, 0, at_rows, at] = jnp.where(place < 2, hx, pltpu.roll(hz, 2, 0))
                    field_ref[parity, 1, at_rows, at] = jnp.where(place < 2, hy, pltpu.roll(hz, 1, 0))

            def top():
                for part, (sym, at) in enumerate(both):
                    rise, fall = zero, zero
                    for pair in range(PAIRS):
                        x, y, _ = load(pair, at)
                        e = pack_ref[0, pair] * (sym["top_x"] * x + sym["top_y"] * y)
                        move = sym["near"] * e
                        turned = turn(move)
                        rise = rise + jnp.where(low_rows, 0.0, turned)
                        keep_ref[pair, part, 0] = (1.0 - sym["self_z"]) * e + rise
                        keep_ref[pair, part, 1] = move
                        rise = (
                            sym["double"] * rise
                            + sym["step"] * move
                            + jnp.where(low_rows, turned, 0.0)
                        )
                    for pair in reversed(range(PAIRS)):
                        move = keep_ref[pair, part, 1]
                        turned = turn(move)
                        fall = fall + jnp.where(low_rows, turned, 0.0)
                        psi = sym["scale"] * (keep_ref[pair, part, 0] + fall)
                        fall = (
                            sym["double"] * fall
                            + sym["step"] * move
                            + jnp.where(low_rows, 0.0, turned)
                        )
                        at_rows = slice(8 * pair, 8 * pair + 8)
                        for half, key in enumerate(("top_x", "top_y")):
                            field_ref[parity, half, at_rows, at] -= jnp.where(
                                place < 2, sym[key] * psi, 0.0
                            )

            if parity == 0 and tile == 0:
                top()
            elif slot == 0:
                pl.when(device == 0)(top)

    for parity in range(2):
        spec_ref[parity] = product(
            split(field_ref[parity].reshape(2 * 8 * PAIRS, HALF)),
            (high_ref[parity], low_ref[parity]),
            NN,
        ).reshape(2, 8 * PAIRS, HALF)

    def scatter(pair, carry):
        at = pl.ds(pl.multiple_of(pair * 8, 8), 8)
        for group in range(4):
            columns = slice(128 * group, 128 * group + 128)
            even = [spec_ref[0, half, at, columns] for half in range(2)]
            odd = [spec_ref[1, half, at, columns] for half in range(2)]
            for far in range(2):
                one, two = (e - o if far else e + o for e, o in zip(even, odd))
                block = slot * BLOCKS + pair * LAYERS + 8 * far + 2 * group
                out_ref[block] = jnp.where(low_half, one, pltpu.roll(two, 64, 1))
                out_ref[block + 1] = jnp.where(low_half, pltpu.roll(one, 64, 1), two)
        return carry

    lax.fori_loop(0, PAIRS, scatter, 0, unroll=2)


def inverse_x(slot, in_ref, high_ref, low_ref):
    low_half = lane_low((DEVICES, 128))
    ref = flat(in_ref)
    one, two, up = (ref[pl.ds(4 * slot + row, DEVICES, stride=8), :] for row in range(3))
    if slot == 0:
        first = lax.broadcasted_iota(jnp.int32, (DEVICES, 128), 0) == 0
        x_one, x_two = jnp.where(first, two, one), jnp.where(first, one, two)
    else:
        x_one, x_two = one, two
    cosine = jnp.concatenate([jnp.where(low_half, x_one, two), pltpu.roll(up, 64, 1)], axis=1)
    sine = jnp.concatenate([jnp.where(low_half, x_two, -one), -up], axis=1)
    waves = jnp.concatenate([cosine, sine], axis=0)
    return product(split(waves), (high_ref[slot], low_ref[slot]), TN)


def relax(damping, magnet_ref, even_ref, odd, out_ref):
    for far in range(2):
        at = slice(HALF * far, HALF * far + HALF)
        field = even_ref[...] - odd if far else even_ref[...] + odd
        h = [field[ROWS * c : ROWS * c + ROWS] for c in range(3)]
        m = [magnet_ref[ROWS * c : ROWS * c + ROWS, at] for c in range(3)]
        p = [m[c - 2] * h[c - 1] - m[c - 1] * h[c - 2] for c in range(3)]
        for c in range(3):
            double = m[c - 2] * p[c - 1] - m[c - 1] * p[c - 2]
            out_ref[ROWS * c : ROWS * c + ROWS, at] = p[c] + damping * double


def kernel(
    sat_ref,
    stiff_ref,
    damping_ref,
    sign_ref,
    magnet_hbm,
    high_hbm,
    low_hbm,
    out_ref,
    magnet_ref,
    high_ref,
    low_ref,
    send_one,
    recv_one,
    send_two,
    recv_two,
    trait_ref,
    pack_ref,
    spec_ref,
    field_ref,
    keep_ref,
    even_ref,
    load_sems,
    send_sems,
    recv_sems,
    ready,
):
    layer, row = lax.axis_index("layer"), lax.axis_index("row")
    me = layer * LAYERS + row
    pair, odd_layer = layer // 2, lax.rem(layer, 2)
    home = pair * LAYERS + row

    def turned(index, by):
        return jnp.bitwise_and(index + by, LAYERS - 1)

    barrier = pltpu.get_barrier_semaphore()

    def greet(step, carry):
        for target in ((layer, turned(row, step)), (turned(layer, step), row)):
            pl.semaphore_signal(barrier, inc=1, device_id=target, device_id_type=MESH)
        return carry

    lax.fori_loop(1, LAYERS, greet, 0)
    loads = [
        pltpu.make_async_copy(source, target, load_sems.at[index])
        for index, (source, target) in enumerate(
            ((magnet_hbm, magnet_ref), (high_hbm, high_ref), (low_hbm, low_ref))
        )
    ]
    for load in loads:
        load.start()
    kinds = lax.broadcasted_iota(jnp.int32, TILE, 0)
    traits = jnp.where(kinds == 0, sat_ref[0], stiff_ref[0])
    traits = jnp.where(kinds == 2, sign_ref[0, 0].astype(F32), traits)
    trait_ref[layer] = jnp.where(kinds == 3, sign_ref[0, 1].astype(F32), traits)
    for load in loads:
        load.wait()
    forward_x(magnet_ref, high_ref, low_ref, send_one, 0)
    pl.semaphore_wait(barrier, 2 * (LAYERS - 1))

    def vouch(step, carry):
        target = (turned(layer, step), row)
        pl.semaphore_signal(ready, inc=1, device_id=target, device_id_type=MESH)
        return carry

    lax.fori_loop(1, LAYERS, vouch, 0)
    forward_x(magnet_ref, high_ref, low_ref, send_one, 1)
    pl.semaphore_wait(ready, LAYERS - 1)

    def push(source, target, index, device_id):
        pltpu.make_async_remote_copy(
            src_ref=source,
            dst_ref=target,
            send_sem=send_sems.at[index],
            recv_sem=recv_sems.at[index],
            device_id=device_id,
            device_id_type=MESH,
        ).start()

    def tell(step, carry):
        push(trait_ref.at[layer], trait_ref.at[layer], 4, (turned(layer, step), row))
        return carry

    def place_of(index):
        return jnp.right_shift(index, 4), jnp.bitwise_and(index, LAYERS - 1)

    def out_first(slot, parity):
        lands = recv_one.at[slot * BLOCKS + home, pl.ds(4 * parity, USED)]

        def step_to(step, carry):
            other = jnp.bitwise_and(me + step, DEVICES - 1)
            push(send_one.at[other, pl.ds(4 * slot, USED)], lands, slot, place_of(other))
            return carry

        lax.fori_loop(1, DEVICES, step_to, 0)
        recv_one[slot * BLOCKS + home, 4 * parity : 4 * parity + USED, :] = send_one[
            me, 4 * slot : 4 * slot + USED, :
        ]

    def out_second(slot, parity):
        lands = recv_two.at[me, pl.ds(4 * slot, USED)]
        for target in (parity, 1 - parity):

            def step_to(step, carry):
                block = jnp.bitwise_and(home + step, BLOCKS - 1)
                other, other_row = place_of(block)
                push(
                    send_two.at[slot * BLOCKS + block, pl.ds(4 * target, USED)],
                    lands,
                    2 + slot,
                    (2 * other + target, other_row),
                )
                return carry

            lax.fori_loop(1 if target == parity else 0, BLOCKS, step_to, 0)
        recv_two[me, 4 * slot : 4 * slot + USED, :] = send_two[
            slot * BLOCKS + home, 4 * parity : 4 * parity + USED, :
        ]

    def by_parity(function, slot):
        for parity in range(2):
            pl.when(odd_layer == parity)(functools.partial(function, slot, parity))

    def drain(ref, sems, index, count):
        every = ref.at[pl.ds(0, count), pl.ds(0, USED)]
        pltpu.make_async_copy(every, every, sems.at[index]).wait()

    def drain_traits(sems):
        every = trait_ref.at[pl.ds(0, LAYERS - 1)]
        pltpu.make_async_copy(every, every, sems.at[4]).wait()

    lax.fori_loop(1, LAYERS, tell, 0)
    for slot in range(2):
        by_parity(out_first, slot)
    drain_traits(recv_sems)
    pack_traits(trait_ref, pack_ref)
    for slot in range(2):
        drain(recv_one, recv_sems, slot, DEVICES - 1)
        couple(
            slot, recv_one, high_ref, low_ref, send_two, pack_ref, spec_ref, field_ref, keep_ref
        )
        by_parity(out_second, slot)
    drain(recv_two, recv_sems, 2, DEVICES - 1)
    even_ref[...] = inverse_x(0, recv_two, high_ref, low_ref)
    for slot in range(2):
        drain(send_one, send_sems, slot, DEVICES - 1)
        drain(send_two, send_sems, 2 + slot, DEVICES - 1)
    drain_traits(send_sems)
    drain(recv_two, recv_sems, 3, DEVICES - 1)
    odd = inverse_x(1, recv_two, high_ref, low_ref)
    relax(damping_ref[0], magnet_ref, even_ref, odd, out_ref)


def on_device(magnet, saturation, stiffness, damping, interface_sign):
    rows = magnet.reshape(3 * ROWS, N)
    spaces = [pltpu.SMEM] * 4 + [pl.ANY] * 3
    buffer, spectrum = (DEVICES, 8, 128), (2, 2, 8 * PAIRS, HALF)
    table = pltpu.VMEM((2, HALF, HALF), BF16)
    shapes = [buffer] * 4 + [(LAYERS, *TILE), (4, PAIRS, *TILE), spectrum, spectrum]
    shapes += [(PAIRS, 2, 4, *TILE), (DEVICES, HALF)]
    torque = pl.pallas_call(
        kernel,
        out_shape=jax.ShapeDtypeStruct(rows.shape, F32),
        in_specs=[pl.BlockSpec(memory_space=space) for space in spaces],
        out_specs=pl.BlockSpec(memory_space=pltpu.VMEM),
        scratch_shapes=[pltpu.VMEM(rows.shape, F32), table, table]
        + [pltpu.VMEM(shape, F32) for shape in shapes]
        + [pltpu.SemaphoreType.DMA((3,))]
        + [pltpu.SemaphoreType.DMA((5,))] * 2
        + [pltpu.SemaphoreType.REGULAR],
        compiler_params=pltpu.CompilerParams(collective_id=0, has_side_effects=True),
        name="torque",
    )(saturation, stiffness, damping, interface_sign, rows, *wave_tables())
    factor = -1.0 / (1.0 + damping * damping)
    return (torque * factor).reshape(magnet.shape)


def solution(mesh):
    in_specs = (P(None, "layer", "row", None), P("layer"), P("layer"), P("layer"), P("layer", None))
    out_specs = P(None, "layer", "row", None)
    return jax.shard_map(
        on_device, mesh=mesh, in_specs=in_specs, out_specs=out_specs, check_vma=False
    )
```

```python
import functools
import math

import jax
import jax.numpy as jnp
import numpy as np
from jax import lax
from jax.experimental import pallas as pl
from jax.experimental.pallas import tpu as pltpu
from jax.sharding import PartitionSpec as P

N = 1024
HALF = N // 2
BINS = N // 4
LAYERS = 16
ROWS = 64
DEVICES = 256
THICKNESS = 1.0
LAYER_PITCH = 1.5
RKKY_STRENGTH = 0.8
F32 = jnp.float32
BF16 = jnp.bfloat16
NT = (((1,), (1,)), ((), ()))
NN = (((1,), (0,)), ((), ()))
TN = (((0,), (0,)), ((), ()))
USED = 3
PAIRS = LAYERS // 2
BLOCKS = DEVICES // 2
TILE = (8, 128)
MESH = pl.DeviceIdType.MESH


def wave_tables():
    grid = np.arange(HALF)
    bins = np.arange(BINS)
    tables = []
    for parity in range(2):
        phase = (2 * bins[:, None] + parity) * grid[None, :] % N * (2.0 * np.pi / N)
        cosines, sines = np.cos(phase), np.sin(phase)
        if parity == 0:
            sines[0] = 1.0 - 2.0 * (grid % 2)
        tables.append(np.concatenate([cosines, sines], axis=0))
    exact = np.stack(tables)
    high = exact.astype(np.dtype(BF16))
    low = (exact - high.astype(np.float64)).astype(np.dtype(BF16))
    return jnp.asarray(high), jnp.asarray(low)


def split(value):
    high = value.astype(BF16)
    return high, (value - high.astype(F32)).astype(BF16)


def product(left, right, dims):
    (left_high, left_low), (right_high, right_low) = left, right
    dot = functools.partial(lax.dot_general, dimension_numbers=dims, preferred_element_type=F32)
    return dot(left_high, right_high) + (dot(left_high, right_low) + dot(left_low, right_high))


def lane_low(shape):
    return lax.broadcasted_iota(jnp.int32, shape, len(shape) - 1) < ROWS


def flat(ref):
    return ref.reshape(ref.shape[0] * 8, 128)


def forward_x(magnet_ref, high_ref, low_ref, out_ref, slot):
    left, right = magnet_ref[:, :HALF], magnet_ref[:, HALF:]
    low_half = lane_low((DEVICES, 128))
    folded = left - right if slot else left + right
    folded = jnp.concatenate([folded, folded[2 * ROWS :]], axis=0)
    waves = product((high_ref[slot], low_ref[slot]), split(folded), NT)
    cosine, sine = waves[:BINS], waves[BINS:]
    one, two = cosine[:, :128], sine[:, :128]
    if slot == 0:
        first = lax.broadcasted_iota(jnp.int32, (DEVICES, 128), 0) == 0
        x_one, x_two = jnp.where(first, two, one), jnp.where(first, one, two)
    else:
        x_one, x_two = one, two
    out = flat(out_ref)
    out[pl.ds(4 * slot, DEVICES, stride=8), :] = jnp.where(low_half, x_one, -two)
    out[pl.ds(4 * slot + 1, DEVICES, stride=8), :] = jnp.where(low_half, x_two, one)
    out[pl.ds(4 * slot + 2, DEVICES, stride=8), :] = jnp.where(
        low_half, -sine[:, 128:], cosine[:, 128:]
    )


def symbols(device, slot, parity, tile, sine):
    bin_y = 2 * (lax.broadcasted_iota(jnp.int32, TILE, 1) + 128 * tile) + parity
    if sine and parity == 0:
        bin_y = jnp.where(bin_y == 0, HALF, bin_y)
    bin_x = jnp.full(TILE, 2 * device + slot, jnp.int32)
    if slot == 0:
        word = lax.broadcasted_iota(jnp.int32, TILE, 0) % 2
        bin_x = jnp.where(device == 0, jnp.where(word == 0, HALF, 0), bin_x)
    top_x, top_y = bin_x == HALF, bin_y == HALF
    wave_x = bin_x.astype(F32) * (2.0 * math.pi / N)
    wave_y = bin_y.astype(F32) * (2.0 * math.pi / N)
    square = wave_x * wave_x + wave_y * wave_y
    anchor = square == 0.0
    norm = jnp.sqrt(jnp.where(anchor, 1.0, square))
    unit_x = jnp.where(anchor, 0.0, wave_x / norm)
    unit_y = jnp.where(anchor, 0.0, wave_y / norm)
    depth = THICKNESS * norm
    series = 1.0 / 5040.0
    for divisor in (-720.0, 120.0, -24.0, 6.0, -2.0, 1.0):
        series = series * depth + 1.0 / divisor
    ratio = jnp.where(depth < 0.25, series, (1.0 - jnp.exp(-depth)) / depth)
    self_z = jnp.where(anchor, 1.0, ratio)
    near = jnp.where(
        anchor, 0.0, 0.5 * depth * ratio * ratio * jnp.exp(-norm * (LAYER_PITCH - THICKNESS))
    )
    step = jnp.exp(-LAYER_PITCH * norm)
    bend = 2.0 * jnp.cos(wave_x) + 2.0 * jnp.cos(wave_y) - 4.0
    scale_x = jnp.where(jnp.logical_or(bin_x == 0, top_x), 1.0, 2.0)
    scale_y = jnp.where(jnp.logical_or(bin_y == 0, top_y), 1.0, 2.0)
    scale = scale_x * scale_y * (1.0 / (N * N))
    return dict(
        x=jnp.where(top_x, 0.0, unit_x),
        y=jnp.where(top_y, 0.0, unit_y),
        top_x=jnp.where(top_x, -unit_x, 0.0),
        top_y=jnp.where(top_y, unit_y, 0.0),
        self_z=self_z,
        near=near,
        step=step,
        double=step * step,
        bend=bend * scale,
        scale=scale,
    )


def pack_traits(trait_ref, pack_ref):
    low_rows = lax.broadcasted_iota(jnp.int32, TILE, 0) < 4
    for pair in range(PAIRS):
        for kind in range(4):
            low, high = (
                jnp.broadcast_to(trait_ref[layer, kind : kind + 1, :], TILE)
                for layer in (2 * pair, 2 * pair + 1)
            )
            if kind == 2 and pair == 0:
                low = jnp.zeros(TILE, F32)
            if kind == 3 and pair == PAIRS - 1:
                high = jnp.zeros(TILE, F32)
            value = jnp.where(low_rows, low, high)
            pack_ref[kind, pair] = RKKY_STRENGTH * value if kind > 1 else value


def couple(slot, in_ref, high_ref, low_ref, out_ref, pack_ref, spec_ref, field_ref, keep_ref):
    device = lax.axis_index("layer") * LAYERS + lax.axis_index("row")
    low_half = lane_low(TILE)
    rows = lax.broadcasted_iota(jnp.int32, TILE, 0)
    low_rows = rows < 4
    place = jnp.bitwise_and(rows, 3)
    zero = jnp.zeros(TILE, F32)

    def gather(pair, carry):
        at = pl.ds(pl.multiple_of(pair * 8, 8), 8)
        for group in range(4):
            plus, minus = [], []
            for block in (2 * group, 2 * group + 1):
                first = slot * BLOCKS + pair * LAYERS + block
                one, two = in_ref[first], in_ref[first + 8]
                plus.append(one + two)
                minus.append(one - two)
            for parity, (one, two) in enumerate((plus, minus)):
                columns = slice(128 * group, 128 * group + 128)
                spec_ref[parity, 0, at, columns] = jnp.where(low_half, one, pltpu.roll(two, 64, 1))
                spec_ref[parity, 1, at, columns] = jnp.where(low_half, pltpu.roll(one, 64, 1), two)
        return carry

    lax.fori_loop(0, PAIRS, gather, 0, unroll=2)
    for parity in range(2):
        waves = product(
            split(spec_ref[parity].reshape(2 * 8 * PAIRS, HALF)),
            (high_ref[parity], low_ref[parity]),
            NT,
        )
        spec_ref[parity] = waves.reshape(2, 8 * PAIRS, HALF)

    def turn(value):
        return pltpu.roll(value, 4, 0)

    for parity in range(2):
        for tile in range(2):
            both = [
                (
                    symbols(device, slot, parity, tile, sine),
                    slice(BINS * sine + 128 * tile, BINS * sine + 128 * tile + 128),
                )
                for sine in range(2)
            ]

            def load(pair, at):
                at_rows = slice(8 * pair, 8 * pair + 8)
                one, two = spec_ref[parity, 0, at_rows, at], spec_ref[parity, 1, at_rows, at]
                up = jnp.where(place == 0, pltpu.roll(one, 6, 0), pltpu.roll(two, 7, 0))
                return one, two, up

            (cs, cos_at), (ss, sin_at) = both
            rise, last = [zero, zero], [zero, zero]
            for pair in range(PAIRS):
                sat = pack_ref[0, pair]
                (xc, yc, zc), (xs, ys, zs) = load(pair, cos_at), load(pair, sin_at)
                along = (cs["x"] * xc + cs["y"] * ys, ss["x"] * xs - ss["y"] * yc)
                for part, (a, z) in enumerate(zip(along, (zc, zs))):
                    sym = both[part][0]
                    keep_ref[pair, part, 3] = z
                    a, z = sat * a, sat * z
                    up, down = sym["near"] * (a + z), sym["near"] * (a - z)
                    turned = turn(up)
                    if pair:
                        rise[part] = rise[part] + jnp.where(low_rows, 0.0, turned)
                    else:
                        rise[part] = jnp.where(low_rows, 0.0, turned)
                    keep_ref[pair, part, 0] = (1.0 - sym["self_z"]) * a + rise[part]
                    keep_ref[pair, part, 1] = sym["self_z"] * z + rise[part]
                    keep_ref[pair, part, 2] = down
                    rise[part] = (
                        sym["double"] * rise[part]
                        + sym["step"] * up
                        + jnp.where(low_rows, turned, 0.0)
                    )
            fall = [zero, zero]
            for pair in reversed(range(PAIRS)):
                psi, chi = [], []
                for part in range(2):
                    sym = both[part][0]
                    down = keep_ref[pair, part, 2]
                    turned = turn(down)
                    fall[part] = fall[part] + jnp.where(low_rows, turned, 0.0)
                    psi.append(keep_ref[pair, part, 0] + fall[part])
                    chi.append(keep_ref[pair, part, 1] - fall[part])
                    fall[part] = (
                        sym["double"] * fall[part]
                        + sym["step"] * down
                        + jnp.where(low_rows, 0.0, turned)
                    )
                stiff, below, above = (pack_ref[kind, pair] for kind in (1, 2, 3))
                at_rows = slice(8 * pair, 8 * pair + 8)

                def raw(which, part, at):
                    rows_of = slice(8 * which, 8 * which + 8)
                    one, two = (spec_ref[parity, half, rows_of, at] for half in range(2))
                    return one, two, keep_ref[which, part, 3]

                for part, (sym, at) in enumerate(both):
                    here = raw(pair, part, at)
                    before = raw(pair - 1, part, at) if pair else (zero,) * 3
                    after = raw(pair + 1, part, at) if pair < PAIRS - 1 else (zero,) * 3
                    cross = cs["y"] * psi[1] if part == 0 else -ss["y"] * psi[0]
                    field = (-sym["x"] * psi[part], cross, -chi[part])
                    hx, hy, hz = (
                        sym["scale"]
                        * (
                            f
                            + below * turn(jnp.where(low_rows, v, b))
                            + above * turn(jnp.where(low_rows, n, v))
                        )
                        + (stiff * sym["bend"]) * v
                        for f, v, b, n in zip(field, here, before, after)
                    )
                    field_ref[parity, 0, at_rows, at] = jnp.where(place < 2, hx, pltpu.roll(hz, 2, 0))
                    field_ref[parity, 1, at_rows, at] = jnp.where(place < 2, hy, pltpu.roll(hz, 1, 0))

            def top():
                for part, (sym, at) in enumerate(both):
                    rise, fall = zero, zero
                    for pair in range(PAIRS):
                        x, y, _ = load(pair, at)
                        e = pack_ref[0, pair] * (sym["top_x"] * x + sym["top_y"] * y)
                        move = sym["near"] * e
                        turned = turn(move)
                        rise = rise + jnp.where(low_rows, 0.0, turned)
                        keep_ref[pair, part, 0] = (1.0 - sym["self_z"]) * e + rise
                        keep_ref[pair, part, 1] = move
                        rise = (
                            sym["double"] * rise
                            + sym["step"] * move
                            + jnp.where(low_rows, turned, 0.0)
                        )
                    for pair in reversed(range(PAIRS)):
                        move = keep_ref[pair, part, 1]
                        turned = turn(move)
                        fall = fall + jnp.where(low_rows, turned, 0.0)
                        psi = sym["scale"] * (keep_ref[pair, part, 0] + fall)
                        fall = (
                            sym["double"] * fall
                            + sym["step"] * move
                            + jnp.where(low_rows, 0.0, turned)
                        )
                        at_rows = slice(8 * pair, 8 * pair + 8)
                        for half, key in enumerate(("top_x", "top_y")):
                            field_ref[parity, half, at_rows, at] -= jnp.where(
                                place < 2, sym[key] * psi, 0.0
                            )

            if parity == 0 and tile == 0:
                top()
            elif slot == 0:
                pl.when(device == 0)(top)

    for parity in range(2):
        spec_ref[parity] = product(
            split(field_ref[parity].reshape(2 * 8 * PAIRS, HALF)),
            (high_ref[parity], low_ref[parity]),
            NN,
        ).reshape(2, 8 * PAIRS, HALF)

    def scatter(pair, carry):
        at = pl.ds(pl.multiple_of(pair * 8, 8), 8)
        for group in range(4):
            columns = slice(128 * group, 128 * group + 128)
            even = [spec_ref[0, half, at, columns] for half in range(2)]
            odd = [spec_ref[1, half, at, columns] for half in range(2)]
            for far in range(2):
                one, two = (e - o if far else e + o for e, o in zip(even, odd))
                block = slot * BLOCKS + pair * LAYERS + 8 * far + 2 * group
                out_ref[block] = jnp.where(low_half, one, pltpu.roll(two, 64, 1))
                out_ref[block + 1] = jnp.where(low_half, pltpu.roll(one, 64, 1), two)
        return carry

    lax.fori_loop(0, PAIRS, scatter, 0, unroll=2)


def inverse_x(slot, in_ref, high_ref, low_ref):
    low_half = lane_low((DEVICES, 128))
    ref = flat(in_ref)
    one, two, up = (ref[pl.ds(4 * slot + row, DEVICES, stride=8), :] for row in range(3))
    if slot == 0:
        first = lax.broadcasted_iota(jnp.int32, (DEVICES, 128), 0) == 0
        x_one, x_two = jnp.where(first, two, one), jnp.where(first, one, two)
    else:
        x_one, x_two = one, two
    cosine = jnp.concatenate([jnp.where(low_half, x_one, two), pltpu.roll(up, 64, 1)], axis=1)
    sine = jnp.concatenate([jnp.where(low_half, x_two, -one), -up], axis=1)
    waves = jnp.concatenate([cosine, sine], axis=0)
    return product(split(waves), (high_ref[slot], low_ref[slot]), TN)


def relax(damping, magnet_ref, even_ref, odd, out_ref):
    for far in range(2):
        at = slice(HALF * far, HALF * far + HALF)
        field = even_ref[...] - odd if far else even_ref[...] + odd
        h = [field[ROWS * c : ROWS * c + ROWS] for c in range(3)]
        m = [magnet_ref[ROWS * c : ROWS * c + ROWS, at] for c in range(3)]
        p = [m[c - 2] * h[c - 1] - m[c - 1] * h[c - 2] for c in range(3)]
        for c in range(3):
            double = m[c - 2] * p[c - 1] - m[c - 1] * p[c - 2]
            out_ref[ROWS * c : ROWS * c + ROWS, at] = p[c] + damping * double


def kernel(
    sat_hbm,
    stiff_hbm,
    damping_hbm,
    sign_hbm,
    magnet_hbm,
    high_hbm,
    low_hbm,
    out_ref,
    sat_ref,
    stiff_ref,
    damping_ref,
    sign_ref,
    magnet_ref,
    high_ref,
    low_ref,
    send_one,
    recv_one,
    send_two,
    recv_two,
    trait_ref,
    pack_ref,
    spec_ref,
    field_ref,
    keep_ref,
    even_ref,
    load_sems,
    send_sems,
    recv_sems,
    ready,
):
    layer, row = lax.axis_index("layer"), lax.axis_index("row")
    me = layer * LAYERS + row
    pair, odd_layer = layer // 2, lax.rem(layer, 2)
    home = pair * LAYERS + row

    def turned(index, by):
        return jnp.bitwise_and(index + by, LAYERS - 1)

    def facing(step):
        return jnp.bitwise_xor(layer, step)

    barrier = pltpu.get_barrier_semaphore()

    def greet(step, carry):
        for target in ((layer, turned(row, step)), (facing(step), row)):
            pl.semaphore_signal(barrier, inc=1, device_id=target, device_id_type=MESH)
        return carry

    lax.fori_loop(1, LAYERS, greet, 0)
    sources = (sat_hbm, stiff_hbm, damping_hbm, sign_hbm, magnet_hbm, high_hbm, low_hbm)
    targets = (sat_ref, stiff_ref, damping_ref, sign_ref, magnet_ref, high_ref, low_ref)
    loads = [
        pltpu.make_async_copy(source, target, load_sems.at[index])
        for index, (source, target) in enumerate(zip(sources, targets))
    ]
    for load in loads:
        load.start()
    pl.semaphore_wait(barrier, 2 * (LAYERS - 1))

    def vouch(step, carry):
        target = (facing(step), row)
        pl.semaphore_signal(ready.at[step], inc=1, device_id=target, device_id_type=MESH)
        return carry

    lax.fori_loop(1, LAYERS, vouch, 0)
    for load in loads:
        load.wait()
    kinds = lax.broadcasted_iota(jnp.int32, TILE, 0)
    traits = jnp.where(kinds == 0, sat_ref[0], stiff_ref[0])
    traits = jnp.where(kinds == 2, sign_ref[0].astype(F32), traits)
    trait_ref[layer] = jnp.where(kinds == 3, sign_ref[1].astype(F32), traits)

    def push(source, target, index, device_id):
        pltpu.make_async_remote_copy(
            src_ref=source,
            dst_ref=target,
            send_sem=send_sems.at[index],
            recv_sem=recv_sems.at[index],
            device_id=device_id,
            device_id_type=MESH,
        ).start()

    def tell(step, carry):
        push(trait_ref.at[layer], trait_ref.at[layer], 4, (facing(step), row))
        return carry

    def place_of(index):
        return jnp.right_shift(index, 4), jnp.bitwise_and(index, LAYERS - 1)

    def out_first(slot, parity):
        lands = recv_one.at[slot * BLOCKS + home, pl.ds(4 * parity, USED)]

        def to_row(other, step, carry):
            other_row = turned(row, step)
            source = send_one.at[other * LAYERS + other_row, pl.ds(4 * slot, USED)]
            push(source, lands, slot, (other, other_row))
            return carry

        lax.fori_loop(1, LAYERS, functools.partial(to_row, layer), 0, unroll=5)

        def to_layer(step, carry):
            if slot == 0:
                pl.semaphore_wait(ready.at[step], 1)
            other = facing(step)
            return lax.fori_loop(0, LAYERS, functools.partial(to_row, other), carry, unroll=4)

        lax.fori_loop(1, LAYERS, to_layer, 0)
        recv_one[slot * BLOCKS + home, 4 * parity : 4 * parity + USED, :] = send_one[
            me, 4 * slot : 4 * slot + USED, :
        ]

    def out_second(slot, parity):
        lands = recv_two.at[me, pl.ds(4 * slot, USED)]
        for target in (parity, 1 - parity):

            def step_to(step, carry):
                block = jnp.bitwise_and(home + step, BLOCKS - 1)
                other, other_row = place_of(block)
                push(
                    send_two.at[slot * BLOCKS + block, pl.ds(4 * target, USED)],
                    lands,
                    2 + slot,
                    (2 * other + target, other_row),
                )
                return carry

            if target == parity:
                lax.fori_loop(1, 4, step_to, 0, unroll=3)
            lax.fori_loop(4 if target == parity else 0, BLOCKS, step_to, 0, unroll=4)
        recv_two[me, 4 * slot : 4 * slot + USED, :] = send_two[
            slot * BLOCKS + home, 4 * parity : 4 * parity + USED, :
        ]

    def by_parity(function, slot):
        for parity in range(2):
            pl.when(odd_layer == parity)(functools.partial(function, slot, parity))

    def drain(ref, sems, index, count):
        every = ref.at[pl.ds(0, count), pl.ds(0, USED)]
        pltpu.make_async_copy(every, every, sems.at[index]).wait()

    def drain_traits(sems):
        every = trait_ref.at[pl.ds(0, LAYERS - 1)]
        pltpu.make_async_copy(every, every, sems.at[4]).wait()

    forward_x(magnet_ref, high_ref, low_ref, send_one, 0)
    lax.fori_loop(1, LAYERS, tell, 0)
    by_parity(out_first, 0)
    forward_x(magnet_ref, high_ref, low_ref, send_one, 1)
    by_parity(out_first, 1)
    drain_traits(recv_sems)
    pack_traits(trait_ref, pack_ref)
    for slot in range(2):
        drain(recv_one, recv_sems, slot, DEVICES - 1)
        couple(
            slot, recv_one, high_ref, low_ref, send_two, pack_ref, spec_ref, field_ref, keep_ref
        )
        by_parity(out_second, slot)
    drain(recv_two, recv_sems, 2, DEVICES - 1)
    even_ref[...] = inverse_x(0, recv_two, high_ref, low_ref)
    for slot in range(2):
        drain(send_one, send_sems, slot, DEVICES - 1)
        drain(send_two, send_sems, 2 + slot, DEVICES - 1)
    drain_traits(send_sems)
    drain(recv_two, recv_sems, 3, DEVICES - 1)
    odd = inverse_x(1, recv_two, high_ref, low_ref)
    relax(damping_ref[0], magnet_ref, even_ref, odd, out_ref)


def on_device(magnet, saturation, stiffness, damping, interface_sign):
    rows = magnet.reshape(3 * ROWS, N)
    buffer, spectrum = (DEVICES, 8, 128), (2, 2, 8 * PAIRS, HALF)
    table = pltpu.VMEM((2, HALF, HALF), BF16)
    shapes = [buffer] * 4 + [(LAYERS, *TILE), (4, PAIRS, *TILE), spectrum, spectrum]
    shapes += [(PAIRS, 2, 4, *TILE), (DEVICES, HALF)]
    torque = pl.pallas_call(
        kernel,
        out_shape=jax.ShapeDtypeStruct(rows.shape, F32),
        in_specs=[pl.BlockSpec(memory_space=pltpu.HBM)] * 7,
        out_specs=pl.BlockSpec(memory_space=pltpu.VMEM),
        scratch_shapes=[pltpu.SMEM((1,), F32)] * 3
        + [pltpu.SMEM((2,), jnp.int32), pltpu.VMEM(rows.shape, F32), table, table]
        + [pltpu.VMEM(shape, F32) for shape in shapes]
        + [pltpu.SemaphoreType.DMA((7,))]
        + [pltpu.SemaphoreType.DMA((5,))] * 2
        + [pltpu.SemaphoreType.REGULAR((LAYERS,))],
        compiler_params=pltpu.CompilerParams(
            collective_id=0, has_side_effects=True, vmem_limit_bytes=53 * 1024 * 1024
        ),
        name="torque",
    )(saturation, stiffness, damping, interface_sign.reshape(2), rows, *wave_tables())
    factor = -1.0 / (1.0 + damping * damping)
    return (torque * factor).reshape(magnet.shape)


def solution(mesh):
    in_specs = (P(None, "layer", "row", None), P("layer"), P("layer"), P("layer"), P("layer", None))
    out_specs = P(None, "layer", "row", None)
    return jax.shard_map(
        on_device, mesh=mesh, in_specs=in_specs, out_specs=out_specs, check_vma=False
    )
```

```python
import functools
import math

import jax
import jax.numpy as jnp
import numpy as np
from jax import lax
from jax.experimental import pallas as pl
from jax.experimental.pallas import tpu as pltpu
from jax.sharding import PartitionSpec as P

N = 1024
HALF = N // 2
BINS = N // 4
LAYERS = 16
ROWS = 64
DEVICES = 256
THICKNESS = 1.0
LAYER_PITCH = 1.5
RKKY_STRENGTH = 0.8
F32 = jnp.float32
BF16 = jnp.bfloat16
NT = (((1,), (1,)), ((), ()))
NN = (((1,), (0,)), ((), ()))
TN = (((0,), (0,)), ((), ()))
USED = 3
PAIRS = LAYERS // 2
BLOCKS = DEVICES // 2
TILE = (8, 128)
MESH = pl.DeviceIdType.MESH


def wave_tables():
    grid = np.arange(HALF)
    bins = np.arange(BINS)
    tables = []
    for parity in range(2):
        phase = (2 * bins[:, None] + parity) * grid[None, :] % N * (2.0 * np.pi / N)
        cosines, sines = np.cos(phase), np.sin(phase)
        if parity == 0:
            sines[0] = 1.0 - 2.0 * (grid % 2)
        tables.append(np.concatenate([cosines, sines], axis=0))
    exact = np.stack(tables)
    high = exact.astype(np.dtype(BF16))
    low = (exact - high.astype(np.float64)).astype(np.dtype(BF16))
    return jnp.asarray(high), jnp.asarray(low)


def split(value):
    high = value.astype(BF16)
    return high, (value - high.astype(F32)).astype(BF16)


def product(left, right, dims):
    (left_high, left_low), (right_high, right_low) = left, right
    dot = functools.partial(lax.dot_general, dimension_numbers=dims, preferred_element_type=F32)
    return dot(left_high, right_high) + (dot(left_high, right_low) + dot(left_low, right_high))


def lane_low(shape):
    return lax.broadcasted_iota(jnp.int32, shape, len(shape) - 1) < ROWS


def flat(ref):
    return ref.reshape(ref.shape[0] * 8, 128)


def forward_x(magnet_ref, high_ref, low_ref, out_ref, slot):
    left, right = magnet_ref[:, :HALF], magnet_ref[:, HALF:]
    low_half = lane_low((DEVICES, 128))
    folded = left - right if slot else left + right
    folded = jnp.concatenate([folded, folded[2 * ROWS :]], axis=0)
    waves = product((high_ref[slot], low_ref[slot]), split(folded), NT)
    cosine, sine = waves[:BINS], waves[BINS:]
    one, two = cosine[:, :128], sine[:, :128]
    if slot == 0:
        first = lax.broadcasted_iota(jnp.int32, (DEVICES, 128), 0) == 0
        x_one, x_two = jnp.where(first, two, one), jnp.where(first, one, two)
    else:
        x_one, x_two = one, two
    out = flat(out_ref)
    out[pl.ds(4 * slot, DEVICES, stride=8), :] = jnp.where(low_half, x_one, -two)
    out[pl.ds(4 * slot + 1, DEVICES, stride=8), :] = jnp.where(low_half, x_two, one)
    out[pl.ds(4 * slot + 2, DEVICES, stride=8), :] = jnp.where(
        low_half, -sine[:, 128:], cosine[:, 128:]
    )


def symbols(device, slot, parity, tile, sine):
    bin_y = 2 * (lax.broadcasted_iota(jnp.int32, TILE, 1) + 128 * tile) + parity
    if sine and parity == 0:
        bin_y = jnp.where(bin_y == 0, HALF, bin_y)
    bin_x = jnp.full(TILE, 2 * device + slot, jnp.int32)
    if slot == 0:
        word = lax.broadcasted_iota(jnp.int32, TILE, 0) % 2
        bin_x = jnp.where(device == 0, jnp.where(word == 0, HALF, 0), bin_x)
    top_x, top_y = bin_x == HALF, bin_y == HALF
    wave_x = bin_x.astype(F32) * (2.0 * math.pi / N)
    wave_y = bin_y.astype(F32) * (2.0 * math.pi / N)
    square = wave_x * wave_x + wave_y * wave_y
    anchor = square == 0.0
    norm = jnp.sqrt(jnp.where(anchor, 1.0, square))
    unit_x = jnp.where(anchor, 0.0, wave_x / norm)
    unit_y = jnp.where(anchor, 0.0, wave_y / norm)
    depth = THICKNESS * norm
    series = 1.0 / 5040.0
    for divisor in (-720.0, 120.0, -24.0, 6.0, -2.0, 1.0):
        series = series * depth + 1.0 / divisor
    ratio = jnp.where(depth < 0.25, series, (1.0 - jnp.exp(-depth)) / depth)
    self_z = jnp.where(anchor, 1.0, ratio)
    near = jnp.where(
        anchor, 0.0, 0.5 * depth * ratio * ratio * jnp.exp(-norm * (LAYER_PITCH - THICKNESS))
    )
    step = jnp.exp(-LAYER_PITCH * norm)
    bend = 2.0 * jnp.cos(wave_x) + 2.0 * jnp.cos(wave_y) - 4.0
    scale_x = jnp.where(jnp.logical_or(bin_x == 0, top_x), 1.0, 2.0)
    scale_y = jnp.where(jnp.logical_or(bin_y == 0, top_y), 1.0, 2.0)
    scale = scale_x * scale_y * (1.0 / (N * N))
    return dict(
        x=jnp.where(top_x, 0.0, unit_x),
        y=jnp.where(top_y, 0.0, unit_y),
        top_x=jnp.where(top_x, -unit_x, 0.0),
        top_y=jnp.where(top_y, unit_y, 0.0),
        self_z=self_z,
        near=near,
        step=step,
        double=step * step,
        bend=bend * scale,
        scale=scale,
    )


def pack_traits(trait_ref, pack_ref):
    low_rows = lax.broadcasted_iota(jnp.int32, TILE, 0) < 4
    for pair in range(PAIRS):
        for kind in range(4):
            low, high = (
                jnp.broadcast_to(trait_ref[layer, kind : kind + 1, :], TILE)
                for layer in (2 * pair, 2 * pair + 1)
            )
            if kind == 2 and pair == 0:
                low = jnp.zeros(TILE, F32)
            if kind == 3 and pair == PAIRS - 1:
                high = jnp.zeros(TILE, F32)
            value = jnp.where(low_rows, low, high)
            pack_ref[kind, pair] = RKKY_STRENGTH * value if kind > 1 else value


def couple(slot, in_ref, high_ref, low_ref, out_ref, pack_ref, spec_ref, field_ref, keep_ref):
    device = lax.axis_index("layer") * LAYERS + lax.axis_index("row")
    low_half = lane_low(TILE)
    rows = lax.broadcasted_iota(jnp.int32, TILE, 0)
    low_rows = rows < 4
    place = jnp.bitwise_and(rows, 3)
    zero = jnp.zeros(TILE, F32)

    def gather(pair, carry):
        at = pl.ds(pl.multiple_of(pair * 8, 8), 8)
        for group in range(4):
            plus, minus = [], []
            for block in (2 * group, 2 * group + 1):
                first = slot * BLOCKS + pair * LAYERS + block
                one, two = in_ref[first], in_ref[first + 8]
                plus.append(one + two)
                minus.append(one - two)
            for parity, (one, two) in enumerate((plus, minus)):
                columns = slice(128 * group, 128 * group + 128)
                spec_ref[parity, 0, at, columns] = jnp.where(low_half, one, pltpu.roll(two, 64, 1))
                spec_ref[parity, 1, at, columns] = jnp.where(low_half, pltpu.roll(one, 64, 1), two)
        return carry

    lax.fori_loop(0, PAIRS, gather, 0, unroll=2)
    for parity in range(2):
        waves = product(
            split(spec_ref[parity].reshape(2 * 8 * PAIRS, HALF)),
            (high_ref[parity], low_ref[parity]),
            NT,
        )
        spec_ref[parity] = waves.reshape(2, 8 * PAIRS, HALF)

    def turn(value):
        return pltpu.roll(value, 4, 0)

    for parity in range(2):
        for tile in range(2):
            both = [
                (
                    symbols(device, slot, parity, tile, sine),
                    slice(BINS * sine + 128 * tile, BINS * sine + 128 * tile + 128),
                )
                for sine in range(2)
            ]

            def load(pair, at):
                at_rows = slice(8 * pair, 8 * pair + 8)
                one, two = spec_ref[parity, 0, at_rows, at], spec_ref[parity, 1, at_rows, at]
                up = jnp.where(place == 0, pltpu.roll(one, 6, 0), pltpu.roll(two, 7, 0))
                return one, two, up

            (cs, cos_at), (ss, sin_at) = both
            rise, last = [zero, zero], [zero, zero]
            for pair in range(PAIRS):
                sat = pack_ref[0, pair]
                (xc, yc, zc), (xs, ys, zs) = load(pair, cos_at), load(pair, sin_at)
                along = (cs["x"] * xc + cs["y"] * ys, ss["x"] * xs - ss["y"] * yc)
                for part, (a, z) in enumerate(zip(along, (zc, zs))):
                    sym = both[part][0]
                    keep_ref[pair, part, 3] = z
                    a, z = sat * a, sat * z
                    up, down = sym["near"] * (a + z), sym["near"] * (a - z)
                    turned = turn(up)
                    if pair:
                        rise[part] = rise[part] + jnp.where(low_rows, 0.0, turned)
                    else:
                        rise[part] = jnp.where(low_rows, 0.0, turned)
                    keep_ref[pair, part, 0] = (1.0 - sym["self_z"]) * a + rise[part]
                    keep_ref[pair, part, 1] = sym["self_z"] * z + rise[part]
                    keep_ref[pair, part, 2] = down
                    rise[part] = (
                        sym["double"] * rise[part]
                        + sym["step"] * up
                        + jnp.where(low_rows, turned, 0.0)
                    )
            fall = [zero, zero]
            for pair in reversed(range(PAIRS)):
                psi, chi = [], []
                for part in range(2):
                    sym = both[part][0]
                    down = keep_ref[pair, part, 2]
                    turned = turn(down)
                    fall[part] = fall[part] + jnp.where(low_rows, turned, 0.0)
                    psi.append(keep_ref[pair, part, 0] + fall[part])
                    chi.append(keep_ref[pair, part, 1] - fall[part])
                    fall[part] = (
                        sym["double"] * fall[part]
                        + sym["step"] * down
                        + jnp.where(low_rows, 0.0, turned)
                    )
                stiff, below, above = (pack_ref[kind, pair] for kind in (1, 2, 3))
                at_rows = slice(8 * pair, 8 * pair + 8)

                def raw(which, part, at):
                    rows_of = slice(8 * which, 8 * which + 8)
                    one, two = (spec_ref[parity, half, rows_of, at] for half in range(2))
                    return one, two, keep_ref[which, part, 3]

                for part, (sym, at) in enumerate(both):
                    here = raw(pair, part, at)
                    before = raw(pair - 1, part, at) if pair else (zero,) * 3
                    after = raw(pair + 1, part, at) if pair < PAIRS - 1 else (zero,) * 3
                    cross = cs["y"] * psi[1] if part == 0 else -ss["y"] * psi[0]
                    field = (-sym["x"] * psi[part], cross, -chi[part])
                    hx, hy, hz = (
                        sym["scale"]
                        * (
                            f
                            + below * turn(jnp.where(low_rows, v, b))
                            + above * turn(jnp.where(low_rows, n, v))
                        )
                        + (stiff * sym["bend"]) * v
                        for f, v, b, n in zip(field, here, before, after)
                    )
                    field_ref[parity, 0, at_rows, at] = jnp.where(place < 2, hx, pltpu.roll(hz, 2, 0))
                    field_ref[parity, 1, at_rows, at] = jnp.where(place < 2, hy, pltpu.roll(hz, 1, 0))

            def top():
                for part, (sym, at) in enumerate(both):
                    rise, fall = zero, zero
                    for pair in range(PAIRS):
                        x, y, _ = load(pair, at)
                        e = pack_ref[0, pair] * (sym["top_x"] * x + sym["top_y"] * y)
                        move = sym["near"] * e
                        turned = turn(move)
                        rise = rise + jnp.where(low_rows, 0.0, turned)
                        keep_ref[pair, part, 0] = (1.0 - sym["self_z"]) * e + rise
                        keep_ref[pair, part, 1] = move
                        rise = (
                            sym["double"] * rise
                            + sym["step"] * move
                            + jnp.where(low_rows, turned, 0.0)
                        )
                    for pair in reversed(range(PAIRS)):
                        move = keep_ref[pair, part, 1]
                        turned = turn(move)
                        fall = fall + jnp.where(low_rows, turned, 0.0)
                        psi = sym["scale"] * (keep_ref[pair, part, 0] + fall)
                        fall = (
                            sym["double"] * fall
                            + sym["step"] * move
                            + jnp.where(low_rows, 0.0, turned)
                        )
                        at_rows = slice(8 * pair, 8 * pair + 8)
                        for half, key in enumerate(("top_x", "top_y")):
                            field_ref[parity, half, at_rows, at] -= jnp.where(
                                place < 2, sym[key] * psi, 0.0
                            )

            if parity == 0 and tile == 0:
                top()
            elif slot == 0:
                pl.when(device == 0)(top)

    for parity in range(2):
        spec_ref[parity] = product(
            split(field_ref[parity].reshape(2 * 8 * PAIRS, HALF)),
            (high_ref[parity], low_ref[parity]),
            NN,
        ).reshape(2, 8 * PAIRS, HALF)

    def scatter(pair, carry):
        at = pl.ds(pl.multiple_of(pair * 8, 8), 8)
        for group in range(4):
            columns = slice(128 * group, 128 * group + 128)
            even = [spec_ref[0, half, at, columns] for half in range(2)]
            odd = [spec_ref[1, half, at, columns] for half in range(2)]
            for far in range(2):
                one, two = (e - o if far else e + o for e, o in zip(even, odd))
                block = slot * BLOCKS + pair * LAYERS + 8 * far + 2 * group
                out_ref[block] = jnp.where(low_half, one, pltpu.roll(two, 64, 1))
                out_ref[block + 1] = jnp.where(low_half, pltpu.roll(one, 64, 1), two)
        return carry

    lax.fori_loop(0, PAIRS, scatter, 0, unroll=2)


def inverse_x(slot, in_ref, high_ref, low_ref):
    low_half = lane_low((DEVICES, 128))
    ref = flat(in_ref)
    one, two, up = (ref[pl.ds(4 * slot + row, DEVICES, stride=8), :] for row in range(3))
    if slot == 0:
        first = lax.broadcasted_iota(jnp.int32, (DEVICES, 128), 0) == 0
        x_one, x_two = jnp.where(first, two, one), jnp.where(first, one, two)
    else:
        x_one, x_two = one, two
    cosine = jnp.concatenate([jnp.where(low_half, x_one, two), pltpu.roll(up, 64, 1)], axis=1)
    sine = jnp.concatenate([jnp.where(low_half, x_two, -one), -up], axis=1)
    waves = jnp.concatenate([cosine, sine], axis=0)
    return product(split(waves), (high_ref[slot], low_ref[slot]), TN)


def relax(damping, magnet_ref, even_ref, odd, out_ref):
    factor = -1.0 / jnp.full((1, 1), 1.0 + damping * damping, F32)
    for far in range(2):
        at = slice(HALF * far, HALF * far + HALF)
        field = even_ref[...] - odd if far else even_ref[...] + odd
        h = [field[ROWS * c : ROWS * c + ROWS] for c in range(3)]
        m = [magnet_ref[ROWS * c : ROWS * c + ROWS, at] for c in range(3)]
        p = [m[c - 2] * h[c - 1] - m[c - 1] * h[c - 2] for c in range(3)]
        for c in range(3):
            double = m[c - 2] * p[c - 1] - m[c - 1] * p[c - 2]
            out_ref[ROWS * c : ROWS * c + ROWS, at] = factor * (p[c] + damping * double)


def kernel(
    sat_hbm,
    stiff_hbm,
    damping_hbm,
    sign_hbm,
    magnet_hbm,
    high_hbm,
    low_hbm,
    out_ref,
    sat_ref,
    stiff_ref,
    damping_ref,
    sign_ref,
    magnet_ref,
    high_ref,
    low_ref,
    send_one,
    recv_one,
    send_two,
    recv_two,
    trait_ref,
    pack_ref,
    spec_ref,
    field_ref,
    keep_ref,
    even_ref,
    load_sems,
    send_sems,
    recv_sems,
    ready,
):
    layer, row = lax.axis_index("layer"), lax.axis_index("row")
    me = layer * LAYERS + row
    pair, odd_layer = layer // 2, lax.rem(layer, 2)
    home = pair * LAYERS + row

    def turned(index, by):
        return jnp.bitwise_and(index + by, LAYERS - 1)

    def facing(step):
        return jnp.bitwise_xor(layer, step)

    barrier = pltpu.get_barrier_semaphore()

    def greet(step, carry):
        for target in ((layer, turned(row, step)), (facing(step), row)):
            pl.semaphore_signal(barrier, inc=1, device_id=target, device_id_type=MESH)
        return carry

    lax.fori_loop(1, LAYERS, greet, 0)
    sources = (sat_hbm, stiff_hbm, damping_hbm, sign_hbm, magnet_hbm, high_hbm, low_hbm)
    targets = (sat_ref, stiff_ref, damping_ref, sign_ref, magnet_ref, high_ref, low_ref)
    loads = [
        pltpu.make_async_copy(source, target, load_sems.at[index])
        for index, (source, target) in enumerate(zip(sources, targets))
    ]
    for load in loads:
        load.start()
    pl.semaphore_wait(barrier, 2 * (LAYERS - 1))

    def vouch(step, carry):
        target = (facing(step), row)
        pl.semaphore_signal(ready.at[step], inc=1, device_id=target, device_id_type=MESH)
        return carry

    lax.fori_loop(1, LAYERS, vouch, 0)
    for load in loads:
        load.wait()
    kinds = lax.broadcasted_iota(jnp.int32, TILE, 0)
    traits = jnp.where(kinds == 0, sat_ref[0], stiff_ref[0])
    traits = jnp.where(kinds == 2, sign_ref[0].astype(F32), traits)
    trait_ref[layer] = jnp.where(kinds == 3, sign_ref[1].astype(F32), traits)

    def push(source, target, index, device_id):
        pltpu.make_async_remote_copy(
            src_ref=source,
            dst_ref=target,
            send_sem=send_sems.at[index],
            recv_sem=recv_sems.at[index],
            device_id=device_id,
            device_id_type=MESH,
        ).start()

    def tell(step, carry):
        push(trait_ref.at[layer], trait_ref.at[layer], 4, (facing(step), row))
        return carry

    def place_of(index):
        return jnp.right_shift(index, 4), jnp.bitwise_and(index, LAYERS - 1)

    def out_first(slot, parity):
        lands = recv_one.at[slot * BLOCKS + home, pl.ds(4 * parity, USED)]

        def to_row(other, step, carry):
            other_row = turned(row, step)
            source = send_one.at[other * LAYERS + other_row, pl.ds(4 * slot, USED)]
            push(source, lands, slot, (other, other_row))
            return carry

        lax.fori_loop(1, LAYERS, functools.partial(to_row, layer), 0, unroll=5)

        def to_layer(step, carry):
            if slot == 0:
                pl.semaphore_wait(ready.at[step], 1)
            other = facing(step)
            return lax.fori_loop(0, LAYERS, functools.partial(to_row, other), carry, unroll=4)

        lax.fori_loop(1, LAYERS, to_layer, 0)
        recv_one[slot * BLOCKS + home, 4 * parity : 4 * parity + USED, :] = send_one[
            me, 4 * slot : 4 * slot + USED, :
        ]

    def out_second(slot, parity):
        lands = recv_two.at[me, pl.ds(4 * slot, USED)]
        for target in (parity, 1 - parity):

            def step_to(step, carry):
                block = jnp.bitwise_and(home + step, BLOCKS - 1)
                other, other_row = place_of(block)
                push(
                    send_two.at[slot * BLOCKS + block, pl.ds(4 * target, USED)],
                    lands,
                    2 + slot,
                    (2 * other + target, other_row),
                )
                return carry

            if target == parity:
                lax.fori_loop(1, 4, step_to, 0, unroll=3)
            lax.fori_loop(4 if target == parity else 0, BLOCKS, step_to, 0, unroll=4)
        recv_two[me, 4 * slot : 4 * slot + USED, :] = send_two[
            slot * BLOCKS + home, 4 * parity : 4 * parity + USED, :
        ]

    def by_parity(function, slot):
        for parity in range(2):
            pl.when(odd_layer == parity)(functools.partial(function, slot, parity))

    def drain(ref, sems, index, count):
        every = ref.at[pl.ds(0, count), pl.ds(0, USED)]
        pltpu.make_async_copy(every, every, sems.at[index]).wait()

    def drain_traits(sems):
        every = trait_ref.at[pl.ds(0, LAYERS - 1)]
        pltpu.make_async_copy(every, every, sems.at[4]).wait()

    forward_x(magnet_ref, high_ref, low_ref, send_one, 0)
    lax.fori_loop(1, LAYERS, tell, 0)
    by_parity(out_first, 0)
    forward_x(magnet_ref, high_ref, low_ref, send_one, 1)
    drain(send_one, send_sems, 0, DEVICES - 1)
    by_parity(out_first, 1)
    drain_traits(recv_sems)
    pack_traits(trait_ref, pack_ref)
    for slot in range(2):
        drain(recv_one, recv_sems, slot, DEVICES - 1)
        couple(
            slot, recv_one, high_ref, low_ref, send_two, pack_ref, spec_ref, field_ref, keep_ref
        )
        by_parity(out_second, slot)
    drain(recv_two, recv_sems, 2, DEVICES - 1)
    even_ref[...] = inverse_x(0, recv_two, high_ref, low_ref)
    for slot in range(2):
        if slot:
            drain(send_one, send_sems, slot, DEVICES - 1)
        drain(send_two, send_sems, 2 + slot, DEVICES - 1)
    drain_traits(send_sems)
    drain(recv_two, recv_sems, 3, DEVICES - 1)
    odd = inverse_x(1, recv_two, high_ref, low_ref)
    relax(damping_ref[0], magnet_ref, even_ref, odd, out_ref)


def on_device(magnet, saturation, stiffness, damping, interface_sign):
    rows = magnet.reshape(3 * ROWS, N)
    buffer, spectrum = (DEVICES, 8, 128), (2, 2, 8 * PAIRS, HALF)
    table = pltpu.VMEM((2, HALF, HALF), BF16)
    shapes = [buffer] * 4 + [(LAYERS, *TILE), (4, PAIRS, *TILE), spectrum, spectrum]
    shapes += [(PAIRS, 2, 4, *TILE), (DEVICES, HALF)]
    torque = pl.pallas_call(
        kernel,
        out_shape=jax.ShapeDtypeStruct(rows.shape, F32),
        in_specs=[pl.BlockSpec(memory_space=pltpu.HBM)] * 7,
        out_specs=pl.BlockSpec(memory_space=pltpu.VMEM),
        scratch_shapes=[pltpu.SMEM((1,), F32)] * 3
        + [pltpu.SMEM((2,), jnp.int32), pltpu.VMEM(rows.shape, F32), table, table]
        + [pltpu.VMEM(shape, F32) for shape in shapes]
        + [pltpu.SemaphoreType.DMA((7,))]
        + [pltpu.SemaphoreType.DMA((5,))] * 2
        + [pltpu.SemaphoreType.REGULAR((LAYERS,))],
        compiler_params=pltpu.CompilerParams(
            collective_id=0, has_side_effects=True, vmem_limit_bytes=53 * 1024 * 1024
        ),
        name="torque",
    )(saturation, stiffness, damping, interface_sign.reshape(2), rows, *wave_tables())
    return torque.reshape(magnet.shape)


def solution(mesh):
    in_specs = (P(None, "layer", "row", None), P("layer"), P("layer"), P("layer"), P("layer", None))
    out_specs = P(None, "layer", "row", None)
    return jax.shard_map(
        on_device, mesh=mesh, in_specs=in_specs, out_specs=out_specs, check_vma=False
    )
```
